128 devices in a mesh: dp: 32 (over x, y, core), mp: 4 (over z).
Axes of the slice: x: 4, y: 4, z: 4, core: 2. Of those that a mesh axis runs over, the one named last changes fastest.
Arguments:
- tokens: bfloat16 [49152, 4096], P('dp'), may hold values from -40 to 40
- norm_gain: bfloat16 [4096], replicated, may hold values from 0.099609375 to 1.8984375
- w_query: bfloat16 [4096, 2048], P(None, 'mp'), may hold values from -1 to 1
- w_key: bfloat16 [4096, 512], P(None, 'mp'), may hold values from -4 to 4
- w_value: bfloat16 [4096, 512], P(None, 'mp'), may hold values from -0.09375 to 0.09375
- w_out: bfloat16 [2048, 4096], P('mp'), may hold values from -0.125 to 0.125
- seq_starts: int32 [256], P('dp'), may hold values from 0 to 1408, as said below
- seq_lengths: int32 [256], P('dp'), may hold values from 128 to 640
- episode_ids: int32 [256], replicated, may hold values from 0 to 3, as said below
- class_ids: int32 [256], replicated, may hold values from 0 to 31
- query_flags: int32 [256], replicated, may hold values from 0 to 1
Outputs:
- log_probs: float32 [256, 32], P('dp')
- prototypes: float32 [128, 4096], P(None, 'mp')
The draws below stay inside these ranges and needn't reach their ends.
Inputs may be any that keep to these rules, and one draw needn't show every extreme that they name: `seq_starts`: slot s lies in the buffer of dp index s // 8; the slots of one buffer are disjoint and in increasing order of start; start plus length is at most 1536, and in every draw the last slot of some buffer ends at row 1536. `episode_ids`: every class of every episode has at least one support sequence.
All inputs are finite; a program needn't handle non-finite values.
Results may differ from the reference program's by a relative error of at most 0.004.
Values sent between devices are 32-bit elements; how exact they have to be, the bound alone decides.
A program may use at most 128 MiB of HBM per device.

```python
import math
import jax
import jax.numpy as jnp
from jax import lax

D = 4096
HEAD_DIM = 128
HEADS = 16
KV_HEADS = 4
WAYS = 32
MIN_LEN = 128
SEQ_DEV = 8
CAP = 1536
NSEQ = 256
EPISODES = 4
CLASSES = 128


def packing(key):
    groups = NSEQ // SEQ_DEV
    subkeys = jax.random.split(jax.random.fold_in(key, 13), 4)
    spare_tokens = CAP - SEQ_DEV * MIN_LEN
    filled = jax.random.randint(subkeys[0], (groups,), 0, spare_tokens + 1)
    fullest = jax.random.randint(subkeys[1], (), 0, groups)
    filled = jnp.where(jnp.arange(groups) == fullest, spare_tokens, filled)
    raw_weights = jax.random.randint(subkeys[2], (groups, 2 * SEQ_DEV), 1, 17)
    weights = raw_weights * raw_weights * raw_weights
    shares = filled[:, None] * weights // jnp.sum(weights, axis=1, keepdims=True)
    remain = filled - jnp.sum(shares, axis=1)
    shares = shares.at[:, 0].add(remain)
    longest_slot = jax.random.randint(subkeys[3], (), 0, SEQ_DEV)
    single = jnp.where(jnp.arange(2 * SEQ_DEV) == longest_slot, spare_tokens, 0)
    shares = jnp.where((jnp.arange(groups) == fullest)[:, None], single[None, :], shares)
    lengths = MIN_LEN + shares[:, :SEQ_DEV]
    gap_sizes = shares[:, SEQ_DEV:]
    extents = lengths + gap_sizes
    starts = jnp.cumsum(extents, axis=1) - extents + gap_sizes
    return (starts.reshape(-1).astype(jnp.int32), lengths.reshape(-1).astype(jnp.int32))


def draw_seq_starts(key, part):
    return packing(key)[0]


def draw_seq_lengths(key, part):
    return packing(key)[1]


def labels(key):
    subkeys = jax.random.split(jax.random.fold_in(key, 7), 3)
    slot_index = jnp.arange(NSEQ, dtype=jnp.int32)
    extra_class = jax.random.randint(subkeys[0], (NSEQ,), 0, CLASSES)
    global_class = jnp.where(slot_index < CLASSES, slot_index, extra_class)
    coin = jax.random.randint(subkeys[1], (NSEQ,), 0, 2)
    asked_flag = jnp.where(slot_index < CLASSES, 0, jnp.where(slot_index == CLASSES, 1, coin))
    shuffle = jax.random.permutation(subkeys[2], NSEQ)
    return (global_class[shuffle], asked_flag[shuffle])


def draw_episode_ids(key, part):
    return (labels(key)[0] // WAYS).astype(jnp.int32)


def draw_class_ids(key, part):
    return (labels(key)[0] % WAYS).astype(jnp.int32)


def draw_query_flags(key, part):
    return labels(key)[1].astype(jnp.int32)


def query_key_pair(key):
    subkeys = jax.random.split(jax.random.fold_in(key, 21), 2)
    query_weight = jax.random.normal(subkeys[0], (D, HEADS * HEAD_DIM), jnp.float32) / math.sqrt(D)
    key_weight = jax.random.normal(subkeys[1], (D, KV_HEADS * HEAD_DIM), jnp.float32) / math.sqrt(D)
    return (jnp.clip(query_weight, -1.0, 1.0), jnp.clip(key_weight, -4.0, 4.0))


def draw_w_query(key, part):
    return query_key_pair(key)[0].astype(jnp.bfloat16)


def draw_w_key(key, part):
    return query_key_pair(key)[1].astype(jnp.bfloat16)


def draw_tokens(key, part):
    row_total = NSEQ // SEQ_DEV * CAP
    subkeys = jax.random.split(jax.random.fold_in(key, 31), 1)
    values = jax.random.normal(subkeys[0], (row_total, D), jnp.float32)
    values = jnp.clip(values, -6.0, 6.0)
    return values.astype(jnp.bfloat16)


def levels(own_key, shape, pieces, smallest, largest):
    level, own = 1.0, jax.random.fold_in(own_key, 6)
    for dim, parts in pieces:
        draws = jnp.exp(jax.random.uniform(jax.random.fold_in(own, dim), (parts,), jnp.float32, smallest / len(pieces), largest / len(pieces)))
        level = level * jnp.repeat(draws, shape[dim] // parts).reshape([-1 if axis == dim else 1 for axis in range(len(shape))])
    return level


def gaussian(key, shape, spread, most, shards=(), kind=jnp.bfloat16):
    entries = spread * jax.random.normal(key, shape, jnp.float32)
    if shards:
        entries = entries * levels(key, shape, shards, -0.22, 0.18)
    return jnp.clip(entries, -most, most).astype(kind)


def setup_inputs(seed: int = 0) -> dict:
    seeds = jax.random.split(jax.random.key(seed), 12)
    return {
        "tokens": draw_tokens(jax.random.fold_in(seeds[11], 71), 0),
        "norm_gain": jnp.clip(1.0 + 0.18 * jax.random.normal(seeds[1], (D,), jnp.float32), 0.099609375, 1.8984375).astype(jnp.bfloat16),
        "w_query": draw_w_query(jax.random.fold_in(seeds[11], 71), 0),
        "w_key": draw_w_key(jax.random.fold_in(seeds[11], 71), 0),
        "w_value": gaussian(seeds[4], (D, KV_HEADS * HEAD_DIM), D ** -0.5, 0.09375, ((1, 4),)),
        "w_out": gaussian(seeds[5], (HEADS * HEAD_DIM, D), (HEADS * HEAD_DIM) ** -0.5, 0.125, ((0, 4),)),
        "seq_starts": draw_seq_starts(jax.random.fold_in(seeds[11], 71), 0),
        "seq_lengths": draw_seq_lengths(jax.random.fold_in(seeds[11], 71), 0),
        "episode_ids": draw_episode_ids(jax.random.fold_in(seeds[11], 71), 0),
        "class_ids": draw_class_ids(jax.random.fold_in(seeds[11], 71), 0),
        "query_flags": draw_query_flags(jax.random.fold_in(seeds[11], 71), 0),
    }


ROPE_BASE = 500000.0
NEG_FILL = -1e+30

def rotate(vectors, positions):
    half_dim = vectors.shape[-1] // 2
    frequency = jnp.power(ROPE_BASE, -(jnp.arange(half_dim, dtype=jnp.float32) * 2.0 / vectors.shape[-1]))
    angles = positions.astype(jnp.float32)[:, None] * frequency[None, :]
    cosine = jnp.cos(angles)[:, None, :]
    sine_part = jnp.sin(angles)[:, None, :]
    leading = vectors[..., :half_dim]
    trailing = vectors[..., half_dim:]
    return jnp.concatenate([leading * cosine - trailing * sine_part, trailing * cosine + leading * sine_part], axis=-1)

def layout_of(starts, lengths, buffer_len):
    token_index = jnp.arange(buffer_len, dtype=jnp.int32)
    inside = (token_index[:, None] >= starts[None, :]) & (token_index[:, None] < (starts + lengths)[None, :])
    slot_number = jnp.arange(starts.shape[0], dtype=jnp.int32)
    segment = lax.optimization_barrier(jnp.sum(jnp.where(inside, slot_number[None, :] + 1, 0), axis=1)).astype(jnp.int32) - 1
    position = lax.optimization_barrier(jnp.sum(jnp.where(inside, token_index[:, None] - starts[None, :], 0), axis=1)).astype(jnp.int32)
    return (segment, position, inside)

def allowed_mask(segment, row_start, row_count, col_count):
    rows_index = row_start + jnp.arange(row_count, dtype=jnp.int32)
    cols_index = jnp.arange(col_count, dtype=jnp.int32)
    seg_rows = segment[row_start:row_start + row_count]
    seg_cols = segment[:col_count]
    same = (seg_rows[:, None] == seg_cols[None, :]) & (seg_rows[:, None] >= 0) & (cols_index[None, :] < rows_index[:, None])
    return (rows_index[:, None] == cols_index[None, :]) | same

def softmax_rows(scores, permitted):
    masked_scores = jnp.where(permitted[None, None], scores, NEG_FILL)
    row_peak = lax.optimization_barrier(jnp.max(masked_scores, axis=-1, keepdims=True))
    exponent = jnp.exp(masked_scores - row_peak)
    totals = lax.optimization_barrier(jnp.sum(exponent, axis=-1, keepdims=True))
    return (exponent / totals).astype(jnp.bfloat16)

def reference(tokens, norm_gain, w_query, w_key, w_value, w_out, seq_starts, seq_lengths, episode_ids, class_ids, query_flags):
    group_count = NSEQ // SEQ_DEV
    group_size = HEADS // KV_HEADS
    inv_root = 1.0 / math.sqrt(HEAD_DIM)
    highest = lax.Precision.HIGHEST

    def embed_group(row_items):
        buffer_rows, starts, lengths = row_items
        segment, position, inside = layout_of(starts, lengths, CAP)
        widened = buffer_rows.astype(jnp.float32)
        normed = (widened * lax.rsqrt(lax.optimization_barrier(jnp.mean(widened * widened, axis=-1, keepdims=True)) + 1e-05) * norm_gain.astype(jnp.float32)).astype(jnp.bfloat16)
        queries = rotate(jnp.dot(normed, w_query, preferred_element_type=jnp.float32).reshape(CAP, HEADS, HEAD_DIM), position).astype(jnp.bfloat16)
        queries = queries.reshape(CAP, KV_HEADS, group_size, HEAD_DIM)
        keys_rot = rotate(jnp.dot(normed, w_key, preferred_element_type=jnp.float32).reshape(CAP, KV_HEADS, HEAD_DIM), position).astype(jnp.bfloat16)
        values_all = jnp.dot(normed, w_value, preferred_element_type=jnp.float32).astype(jnp.bfloat16).reshape(CAP, KV_HEADS, HEAD_DIM)
        scores = jnp.einsum('qngd,knd->ngqk', queries.astype(jnp.float32), keys_rot.astype(jnp.float32), precision=highest) * inv_root
        permitted = allowed_mask(segment, 0, CAP, CAP)
        attention_probs = softmax_rows(scores, permitted)
        attended = jnp.einsum('ngqk,knd->qngd', attention_probs.astype(jnp.float32), values_all.astype(jnp.float32), precision=highest)
        attended = attended.astype(jnp.bfloat16).reshape(CAP, HEADS * HEAD_DIM)
        layer_out = widened + jnp.dot(attended, w_out, preferred_element_type=jnp.float32)
        member = inside.T.astype(jnp.float32)
        return jnp.dot(member, layer_out, precision=highest) / lengths.astype(jnp.float32)[:, None]
    pooled = lax.map(embed_group, (tokens.reshape(group_count, CAP, D), seq_starts.reshape(group_count, SEQ_DEV), seq_lengths.reshape(group_count, SEQ_DEV)))
    pooled = pooled.reshape(NSEQ, D)
    embedded = pooled * lax.rsqrt(lax.optimization_barrier(jnp.mean(pooled * pooled, axis=-1, keepdims=True)) + 1e-06)
    global_class = episode_ids * WAYS + class_ids
    is_support = query_flags == 0
    select_all = ((global_class[None, :] == jnp.arange(CLASSES, dtype=jnp.int32)[:, None]) & is_support[None, :]).astype(jnp.float32)
    class_sums = jnp.dot(select_all, embedded, precision=highest)
    prototypes = class_sums * lax.rsqrt(lax.optimization_barrier(jnp.mean(class_sums * class_sums, axis=-1, keepdims=True)) + 1e-06)
    episode_protos = prototypes.reshape(EPISODES, WAYS, D)

    def score_row(row_items):
        vector, episode = row_items
        chosen = lax.dynamic_index_in_dim(episode_protos, episode, 0, keepdims=False)
        difference = vector[None, :] - chosen
        return lax.optimization_barrier(jnp.sum(difference * difference, axis=-1))
    distance = lax.map(score_row, (embedded, episode_ids))
    logits = -distance / math.sqrt(D)
    row_peak = lax.optimization_barrier(jnp.max(logits, axis=-1, keepdims=True))
    shifted = logits - row_peak
    log_probs = shifted - jnp.log(lax.optimization_barrier(jnp.sum(jnp.exp(shifted), axis=-1, keepdims=True)))
    log_probs = jnp.where(query_flags[:, None] == 1, log_probs, 0.0)
    return (log_probs, prototypes)
```

```python
import functools
import math

import jax
import jax.numpy as jnp
import numpy as np
from jax import lax
from jax.experimental import pallas as pl
from jax.experimental.pallas import tpu as pltpu
from jax.sharding import PartitionSpec as P

HEAD_DIM = 128
WAYS = 32
ROPE_BASE = 500000.0
LONGEST = 640
STEPS = 8
TILE = 128
ONES = 16
FAR = -(2.0**100)
F32 = jnp.float32
BF16 = jnp.bfloat16


def rope_tables(rows, block):
    half = HEAD_DIM // 2
    frequency = ROPE_BASE ** (-(np.arange(half, dtype=np.float64) * 2.0 / HEAD_DIM))
    frequency = np.concatenate([frequency, frequency])[None, :]
    sign = np.where(np.arange(HEAD_DIM) < half, -1.0, 1.0)[None, :]
    fine = np.arange(block, dtype=np.float64)[:, None] * frequency
    coarse = np.arange(0, rows, block, dtype=np.float64)[:, None] * frequency
    fine_table = np.stack([np.cos(fine), np.sin(fine)])
    coarse_table = np.stack(
        [np.cos(coarse), np.sin(coarse), sign * np.cos(coarse), sign * np.sin(coarse)]
    )
    return fine_table.astype(np.float32), coarse_table.astype(np.float32)


def dot(a, b):
    return jnp.dot(a, b, preferred_element_type=F32)


def dot_nt(a, b):
    return lax.dot_general(a, b, (((1,), (1,)), ((), ())), preferred_element_type=F32)


def local_kernel(
    starts,
    lengths,
    gain,
    fine,
    coarse,
    x_ref,
    wq_ref,
    wk_ref,
    wv_ref,
    att_ref,
    tok_ref,
    acc,
    squares,
    member,
    qs,
    ks,
    vt,
    ot,
):
    step = pl.program_id(0)
    rows, depth = x_ref.shape
    slots = starts.shape[0]
    heads = wq_ref.shape[1] // HEAD_DIM
    width = depth * STEPS
    tiles = rows // TILE
    half_rows = rows // 3

    @pl.when(step == 0)
    def _():
        token = lax.broadcasted_iota(jnp.int32, (ONES, rows), 1)
        slot = lax.broadcasted_iota(jnp.int32, (ONES, rows), 0)
        first = jnp.zeros((ONES, rows), jnp.int32)
        last = jnp.zeros((ONES, rows), jnp.int32)
        for s in range(slots):
            first = jnp.where(slot == s, starts[s], first)
            last = jnp.where(slot == s, starts[s] + lengths[s], last)
        member[...] = jnp.where((token >= first) & (token < last), 1.0, 0.0).astype(BF16)

    weights = jnp.concatenate([wq_ref[...], wk_ref[...], wv_ref[...]], axis=1)

    def project(fresh):
        for r in range(3):
            at = pl.ds(r * half_rows, half_rows)
            x = x_ref[at, :]
            wide = x.astype(F32)
            wide = wide * wide
            total = wide[:, 0:128]
            for c in range(1, depth // 128):
                total += wide[:, c * 128 : (c + 1) * 128]
            part = dot(x * gain[...], weights)
            if fresh:
                squares[at, :] = total
                acc[at, :] = part
            else:
                squares[at, :] += total
                acc[at, :] += part

    @pl.when(step == 0)
    def _():
        project(True)

    @pl.when(step > 0)
    def _():
        project(False)

    per_rank = STEPS // lax.axis_size("mp")
    rank = lax.axis_index("mp")

    for c in range(per_rank):

        @pl.when(step == rank * per_rank + c)
        def _():
            tok_ref[:, c * depth : (c + 1) * depth] = dot(member[...], x_ref[...])[:slots]

    @pl.when(step == STEPS - 1)
    def _():
        scale = math.log2(math.e) / math.sqrt(HEAD_DIM)
        lane = lax.broadcasted_iota(jnp.int32, (1, 128), 1)
        first = jnp.full((1, 128), rows, jnp.int32)
        last = jnp.full((1, 128), 0, jnp.int32)
        for s in range(slots):
            first = jnp.where(lane == s, starts[s], first)
            last = jnp.where(lane == s, starts[s] + lengths[s], last)
        fine_cos, fine_sin = fine[0], fine[1]
        for i in range(tiles):
            for h in range(TILE // 64):
                low = i * TILE + h * 64
                at = pl.ds(low, 64)
                row_scale = lax.rsqrt(
                    jnp.sum(squares[at, :], axis=1, keepdims=True) * (1.0 / width) + 1e-05
                )
                block = low // 64
                cos_a, sin_a = coarse[0, block : block + 1, :], coarse[1, block : block + 1, :]
                cos_s, sin_s = coarse[2, block : block + 1, :], coarse[3, block : block + 1, :]
                cosine = (cos_a * fine_cos - sin_a * fine_sin) * row_scale
                sine = (sin_s * fine_cos + cos_s * fine_sin) * row_scale
                token = low + lax.broadcasted_iota(jnp.int32, (64, 128), 0)
                inside = (token >= first) & (token < last)
                q_mark = jnp.where(inside, 1.0, 0.0).astype(BF16)
                k_mark = jnp.where(inside, 0.0, FAR).astype(BF16)
                for n in range(heads):
                    v = acc[at, n * 128 : (n + 1) * 128]
                    v = v * cosine + pltpu.roll(v, 64, 1) * sine
                    to = pl.ds(n * TILE + h * 64, 64)
                    qs[i, to, 0:128] = v.astype(BF16)
                    qs[i, to, 128:256] = q_mark
                v = acc[at, heads * 128 : (heads + 1) * 128] * scale
                v = v * cosine + pltpu.roll(v, 64, 1) * sine
                ks[at, 0:128] = v.astype(BF16)
                ks[at, 128:256] = k_mark
            at = pl.ds(i * TILE, TILE)
            row_scale = lax.rsqrt(
                jnp.sum(squares[at, :], axis=1, keepdims=True) * (1.0 / width) + 1e-05
            )
            v = acc[at, (heads + 1) * 128 : (heads + 2) * 128] * row_scale
            vt[0:128, at] = v.T.astype(BF16)
            vt[128 : 128 + ONES, at] = jnp.ones((ONES, TILE), BF16)
        key = lax.broadcasted_iota(jnp.int32, (TILE, heads * TILE), 0)
        query = lax.broadcasted_iota(jnp.int32, (TILE, heads * TILE), 1) % TILE
        causal = key <= query
        for i in range(tiles):
            begin = max(0, i * TILE - LONGEST)
            count = (i * TILE - begin) // TILE
            scores = []
            for c in range(count + 1):
                s = dot_nt(ks[begin + c * TILE : begin + (c + 1) * TILE, :], qs[i])
                if c == count:
                    s = jnp.where(causal, s, FAR)
                scores.append(s)
            s = jnp.concatenate(scores, axis=0)
            e = jnp.exp2(s - jnp.max(s, axis=0, keepdims=True)).astype(BF16)
            o = dot(vt[:, begin : (i + 1) * TILE], e)
            o = (o[0:128] / o[128:129]).astype(BF16)
            for n in range(heads):
                ot[n * 128 : (n + 1) * 128, i * TILE : (i + 1) * TILE] = o[
                    :, n * TILE : (n + 1) * TILE
                ]
        att_ref[...] = dot_nt(member[...], ot[...])[:slots]


def local_part(tokens, norm_gain, w_query, w_key, w_value, seq_starts, seq_lengths):
    rows, width = tokens.shape
    slots = seq_starts.shape[0]
    heads = w_query.shape[1] // HEAD_DIM
    columns = w_query.shape[1] + w_key.shape[1] + w_value.shape[1]
    depth = width // STEPS
    fine, coarse = rope_tables(rows, 64)
    share = width // lax.axis_size("mp")
    tiles = rows // TILE
    whole = lambda shape: pl.BlockSpec(shape, lambda k: (0,) * len(shape))
    return pl.pallas_call(
        local_kernel,
        grid=(STEPS,),
        out_shape=(
            jax.ShapeDtypeStruct((slots, heads * HEAD_DIM), F32),
            jax.ShapeDtypeStruct((slots, share), F32),
        ),
        in_specs=[
            pl.BlockSpec(memory_space=pltpu.SMEM),
            pl.BlockSpec(memory_space=pltpu.SMEM),
            pl.BlockSpec((1, depth), lambda k: (0, k)),
            whole(fine.shape),
            whole(coarse.shape),
            pl.BlockSpec((rows, depth), lambda k: (0, k)),
            pl.BlockSpec((depth, w_query.shape[1]), lambda k: (k, 0)),
            pl.BlockSpec((depth, w_key.shape[1]), lambda k: (k, 0)),
            pl.BlockSpec((depth, w_value.shape[1]), lambda k: (k, 0)),
        ],
        out_specs=(whole((slots, heads * HEAD_DIM)), whole((slots, share))),
        scratch_shapes=[
            pltpu.VMEM((rows, columns), F32),
            pltpu.VMEM((rows, 128), F32),
            pltpu.VMEM((ONES, rows), BF16),
            pltpu.VMEM((tiles, heads * TILE, 256), BF16),
            pltpu.VMEM((rows, 256), BF16),
            pltpu.VMEM((128 + ONES, rows), BF16),
            pltpu.VMEM((heads * HEAD_DIM, rows), BF16),
        ],
        compiler_params=pltpu.CompilerParams(
            dimension_semantics=("arbitrary",), vmem_limit_bytes=44 * 2**20
        ),
        name="local_part",
    )(
        seq_starts,
        seq_lengths,
        norm_gain.reshape(1, width),
        jnp.asarray(fine),
        jnp.asarray(coarse),
        tokens,
        w_query,
        w_key,
        w_value,
    )


def per_device(
    tokens,
    norm_gain,
    w_query,
    w_key,
    w_value,
    w_out,
    seq_starts,
    seq_lengths,
    episode_ids,
    class_ids,
    query_flags,
):
    width = tokens.shape[1]
    slots = seq_starts.shape[0]
    attended, token_sums = local_part(
        tokens, norm_gain, w_query, w_key, w_value, seq_starts, seq_lengths
    )
    high = attended.astype(BF16)
    low = (attended - high.astype(F32)).astype(BF16)
    both = dot(jnp.concatenate([high, low], axis=0), w_out)
    head_part = both[:slots] + both[slots:]
    mp = lax.axis_size("mp")
    share = width // mp
    pieces = head_part.reshape(slots, mp, share).transpose(1, 0, 2)
    pieces = lax.all_to_all(pieces, "mp", split_axis=0, concat_axis=0, tiled=True)
    pooled = (token_sums + pieces.sum(axis=0)) / seq_lengths.astype(F32)[:, None]
    square = lax.psum(jnp.sum(pooled * pooled, axis=-1, keepdims=True), "mp")
    embedded = pooled * lax.rsqrt(square / width + 1e-06)
    everyone = lax.all_gather(embedded, "dp", axis=0, tiled=True)
    seq_total = episode_ids.shape[0]
    episodes = max(1, seq_total // (2 * WAYS))
    classes = episodes * WAYS
    global_class = episode_ids * WAYS + class_ids
    class_range = jnp.arange(classes, dtype=jnp.int32)
    select = (
        (global_class[None, :] == class_range[:, None]) & (query_flags == 0)[None, :]
    ).astype(F32)
    highest = lax.Precision.HIGHEST
    sums = jnp.dot(select, everyone, precision=highest)
    cross = lax.dot_general(embedded, sums, (((1,), (1,)), ((), ())), precision=highest)
    packed = jnp.concatenate([cross, jnp.sum(sums * sums, axis=1)[None, :]], axis=0)
    packed = lax.psum(packed, "mp")
    mean_square = packed[slots] / width
    scale = lax.rsqrt(mean_square + 1e-06)
    prototypes = sums * scale[:, None]
    own_square = (square / width) / (square / width + 1e-06) * width
    distance = (
        own_square - 2.0 * packed[:slots] * scale[None, :] + (mean_square * scale * scale * width)[None, :]
    )
    own_first = lax.axis_index("dp") * slots
    own_episode = lax.dynamic_slice_in_dim(episode_ids, own_first, slots, 0)
    own_query = lax.dynamic_slice_in_dim(query_flags, own_first, slots, 0)
    picked = jnp.sum(
        jnp.where(
            own_episode[:, None, None] == jnp.arange(episodes, dtype=jnp.int32)[None, :, None],
            distance.reshape(slots, episodes, WAYS),
            0.0,
        ),
        axis=1,
    )
    logits = -picked / math.sqrt(width)
    shifted = logits - jnp.max(logits, axis=-1, keepdims=True)
    log_probs = shifted - jnp.log(jnp.sum(jnp.exp(shifted), axis=-1, keepdims=True))
    return jnp.where(own_query[:, None] == 1, log_probs, 0.0), prototypes


def solution(mesh):
    placed = (
        P("dp", None),
        P(),
        P(None, "mp"),
        P(None, "mp"),
        P(None, "mp"),
        P("mp", None),
        P("dp"),
        P("dp"),
        P(),
        P(),
        P(),
    )
    return jax.shard_map(
        per_device,
        mesh=mesh,
        in_specs=placed,
        out_specs=(P("dp", None), P(None, "mp")),
        check_vma=False,
    )
```

```python
import functools
import math

import jax
import jax.numpy as jnp
import numpy as np
from jax import lax
from jax.experimental import pallas as pl
from jax.experimental.pallas import tpu as pltpu
from jax.sharding import PartitionSpec as P

HEAD_DIM = 128
WAYS = 32
ROPE_BASE = 500000.0
LONGEST = 640
STEPS = 8
TILE = 128
ONES = 16
FAR = -(2.0**100)
F32 = jnp.float32
BF16 = jnp.bfloat16


def rope_tables(rows, block):
    half = HEAD_DIM // 2
    frequency = ROPE_BASE ** (-(np.arange(half, dtype=np.float64) * 2.0 / HEAD_DIM))
    frequency = np.concatenate([frequency, frequency])[None, :]
    sign = np.where(np.arange(HEAD_DIM) < half, -1.0, 1.0)[None, :]
    fine = np.arange(block, dtype=np.float64)[:, None] * frequency
    coarse = np.arange(0, rows, block, dtype=np.float64)[:, None] * frequency
    fine_table = np.stack([np.cos(fine), np.sin(fine)])
    coarse_table = np.stack(
        [np.cos(coarse), np.sin(coarse), sign * np.cos(coarse), sign * np.sin(coarse)]
    )
    return fine_table.astype(np.float32), coarse_table.astype(np.float32)


def dot(a, b):
    return jnp.dot(a, b, preferred_element_type=F32)


def dot_nt(a, b):
    return lax.dot_general(a, b, (((1,), (1,)), ((), ())), preferred_element_type=F32)


def local_kernel(
    starts,
    lengths,
    gain,
    fine,
    coarse,
    x_ref,
    wq_ref,
    wk_ref,
    wv_ref,
    att_ref,
    tok_ref,
    acc,
    squares,
    member,
    qs,
    ks,
    vt,
    ot,
):
    step = pl.program_id(0)
    rows, depth = x_ref.shape
    slots = starts.shape[0]
    heads = wq_ref.shape[1] // HEAD_DIM
    width = depth * STEPS
    tiles = rows // TILE
    half_rows = rows // 3

    @pl.when(step == 0)
    def _():
        token = lax.broadcasted_iota(jnp.int32, (ONES, rows), 1)
        slot = lax.broadcasted_iota(jnp.int32, (ONES, rows), 0)
        first = jnp.zeros((ONES, rows), jnp.int32)
        last = jnp.zeros((ONES, rows), jnp.int32)
        for s in range(slots):
            first = jnp.where(slot == s, starts[s], first)
            last = jnp.where(slot == s, starts[s] + lengths[s], last)
        member[...] = jnp.where((token >= first) & (token < last), 1.0, 0.0).astype(BF16)

    weights = jnp.concatenate([wq_ref[...], wk_ref[...], wv_ref[...]], axis=1)

    def project(fresh):
        for r in range(3):
            at = pl.ds(r * half_rows, half_rows)
            x = x_ref[at, :]
            wide = x.astype(F32)
            wide = wide * wide
            total = wide[:, 0:128]
            for c in range(1, depth // 128):
                total += wide[:, c * 128 : (c + 1) * 128]
            part = dot(x * gain[...], weights)
            if fresh:
                squares[at, :] = total
                acc[at, :] = part
            else:
                squares[at, :] += total
                acc[at, :] += part

    @pl.when(step == 0)
    def _():
        project(True)

    @pl.when(step > 0)
    def _():
        project(False)

    per_rank = STEPS // lax.axis_size("mp")
    rank = lax.axis_index("mp")

    for c in range(per_rank):

        @pl.when(step == rank * per_rank + c)
        def _():
            tok_ref[:, c * depth : (c + 1) * depth] = dot(member[...], x_ref[...])[:slots]

    @pl.when(step == STEPS - 1)
    def _():
        scale = math.log2(math.e) / math.sqrt(HEAD_DIM)
        lane = lax.broadcasted_iota(jnp.int32, (1, 128), 1)
        first = jnp.full((1, 128), rows, jnp.int32)
        last = jnp.full((1, 128), 0, jnp.int32)
        for s in range(slots):
            first = jnp.where(lane == s, starts[s], first)
            last = jnp.where(lane == s, starts[s] + lengths[s], last)
        fine_cos, fine_sin = fine[0], fine[1]
        for i in range(tiles):
            for h in range(TILE // 64):
                low = i * TILE + h * 64
                at = pl.ds(low, 64)
                row_scale = lax.rsqrt(
                    jnp.sum(squares[at, :], axis=1, keepdims=True) * (1.0 / width) + 1e-05
                )
                block = low // 64
                cos_a, sin_a = coarse[0, block : block + 1, :], coarse[1, block : block + 1, :]
                cos_s, sin_s = coarse[2, block : block + 1, :], coarse[3, block : block + 1, :]
                cosine = (cos_a * fine_cos - sin_a * fine_sin) * row_scale
                sine = (sin_s * fine_cos + cos_s * fine_sin) * row_scale
                token = low + lax.broadcasted_iota(jnp.int32, (64, 128), 0)
                inside = (token >= first) & (token < last)
                q_mark = jnp.where(inside, 1.0, 0.0).astype(BF16)
                k_mark = jnp.where(inside, 0.0, FAR).astype(BF16)
                for n in range(heads):
                    v = acc[at, n * 128 : (n + 1) * 128]
                    v = v * cosine + pltpu.roll(v, 64, 1) * sine
                    to = pl.ds(n * TILE + h * 64, 64)
                    qs[i, to, 0:128] = v.astype(BF16)
                    qs[i, to, 128:256] = q_mark
                v = acc[at, heads * 128 : (heads + 1) * 128] * scale
                v = v * cosine + pltpu.roll(v, 64, 1) * sine
                ks[at, 0:128] = v.astype(BF16)
                ks[at, 128:256] = k_mark
            at = pl.ds(i * TILE, TILE)
            row_scale = lax.rsqrt(
                jnp.sum(squares[at, :], axis=1, keepdims=True) * (1.0 / width) + 1e-05
            )
            v = acc[at, (heads + 1) * 128 : (heads + 2) * 128] * row_scale
            vt[0:128, at] = v.T.astype(BF16)
            vt[128 : 128 + ONES, at] = jnp.ones((ONES, TILE), BF16)
        key = lax.broadcasted_iota(jnp.int32, (TILE, heads * TILE), 0)
        query = lax.broadcasted_iota(jnp.int32, (TILE, heads * TILE), 1) % TILE
        causal = key <= query
        for i in range(tiles):
            begin = max(0, i * TILE - LONGEST)
            count = (i * TILE - begin) // TILE
            scores = []
            for c in range(count + 1):
                s = dot_nt(ks[begin + c * TILE : begin + (c + 1) * TILE, :], qs[i])
                if c == count:
                    s = jnp.where(causal, s, FAR)
                scores.append(s)
            s = jnp.concatenate(scores, axis=0)
            e = jnp.exp2(s - jnp.max(s, axis=0, keepdims=True)).astype(BF16)
            o = dot(vt[:, begin : (i + 1) * TILE], e)
            o = (o[0:128] / o[128:129]).astype(BF16)
            for n in range(heads):
                ot[n * 128 : (n + 1) * 128, i * TILE : (i + 1) * TILE] = o[
                    :, n * TILE : (n + 1) * TILE
                ]
        att_ref[...] = dot_nt(member[...], ot[...])[:slots]


def local_part(tokens, norm_gain, w_query, w_key, w_value, seq_starts, seq_lengths):
    rows, width = tokens.shape
    slots = seq_starts.shape[0]
    heads = w_query.shape[1] // HEAD_DIM
    columns = w_query.shape[1] + w_key.shape[1] + w_value.shape[1]
    depth = width // STEPS
    fine, coarse = rope_tables(rows, 64)
    share = width // lax.axis_size("mp")
    tiles = rows // TILE
    whole = lambda shape: pl.BlockSpec(shape, lambda k: (0,) * len(shape))
    return pl.pallas_call(
        local_kernel,
        grid=(STEPS,),
        out_shape=(
            jax.ShapeDtypeStruct((slots, heads * HEAD_DIM), F32),
            jax.ShapeDtypeStruct((slots, share), F32),
        ),
        in_specs=[
            pl.BlockSpec(memory_space=pltpu.SMEM),
            pl.BlockSpec(memory_space=pltpu.SMEM),
            pl.BlockSpec((1, depth), lambda k: (0, k)),
            whole(fine.shape),
            whole(coarse.shape),
            pl.BlockSpec((rows, depth), lambda k: (0, k)),
            pl.BlockSpec((depth, w_query.shape[1]), lambda k: (k, 0)),
            pl.BlockSpec((depth, w_key.shape[1]), lambda k: (k, 0)),
            pl.BlockSpec((depth, w_value.shape[1]), lambda k: (k, 0)),
        ],
        out_specs=(whole((slots, heads * HEAD_DIM)), whole((slots, share))),
        scratch_shapes=[
            pltpu.VMEM((rows, columns), F32),
            pltpu.VMEM((rows, 128), F32),
            pltpu.VMEM((ONES, rows), BF16),
            pltpu.VMEM((tiles, heads * TILE, 256), BF16),
            pltpu.VMEM((rows, 256), BF16),
            pltpu.VMEM((128 + ONES, rows), BF16),
            pltpu.VMEM((heads * HEAD_DIM, rows), BF16),
        ],
        compiler_params=pltpu.CompilerParams(
            dimension_semantics=("arbitrary",), vmem_limit_bytes=44 * 2**20
        ),
        name="local_part",
    )(
        seq_starts,
        seq_lengths,
        norm_gain.reshape(1, width),
        jnp.asarray(fine),
        jnp.asarray(coarse),
        tokens,
        w_query,
        w_key,
        w_value,
    )


def split(a):
    high = a.astype(BF16)
    return high, (a - high.astype(F32)).astype(BF16)


def exchange_kernel(
    lengths,
    episode_s,
    flag_s,
    episode_v,
    class_v,
    flag_v,
    att_ref,
    tok_ref,
    wo_ref,
    log_ref,
    proto_ref,
    part,
    landed,
    everyone,
    square_part,
    square_landed,
    squares,
    final_part,
    final_landed,
    rs_send,
    rs_recv,
    sq_send,
    sq_recv,
    ag_send,
    ag_recv,
    relay_send,
    relay_recv,
    all_send,
    all_recv,
    fin_send,
    fin_recv,
):
    mp = lax.axis_size("mp")
    dp = lax.axis_size("dp")
    me = lax.axis_index("mp")
    mine = lax.axis_index("dp")
    slots = att_ref.shape[0]
    share = tok_ref.shape[1]
    width = share * mp
    side = int(math.isqrt(dp // 2))
    x, y, core = mine // (2 * side), (mine // 2) % side, mine % 2
    partner = mine + 1 - 2 * core

    def at(dx, dy):
        return (((x + dx + side) % side) * side + (y + dy + side) % side) * 2 + core

    barrier = pltpu.get_barrier_semaphore()
    for d in range(1, mp):
        pl.semaphore_signal(barrier, inc=1, device_id={"mp": (me + d) % mp})

    def greet(d, carry):
        pl.semaphore_signal(barrier, inc=1, device_id={"dp": (mine + d) % dp})
        return carry

    lax.fori_loop(1, dp, greet, 0)

    high, low = split(att_ref[...])
    stacked = jnp.concatenate([high, low], axis=0)
    for r in range(mp):
        both = dot(stacked, wo_ref[:, r * share : (r + 1) * share])
        part[r] = both[:slots] + both[slots:]

    pl.semaphore_wait(barrier, mp - 1 + dp - 1)

    order = sorted(range(1, mp), key=lambda d: -min(d, mp - d))
    copies = {}
    for d in order:
        copies[d] = pltpu.make_async_remote_copy(
            src_ref=part.at[(me + d) % mp],
            dst_ref=landed.at[d - 1],
            send_sem=rs_send.at[d - 1],
            recv_sem=rs_recv.at[d - 1],
            device_id={"mp": (me + d) % mp},
        )
        copies[d].start()
    row = lax.broadcasted_iota(jnp.int32, (slots, 1), 0)
    count = jnp.ones((slots, 1), jnp.int32)
    for s in range(slots):
        count = jnp.where(row == s, lengths[s], count)
    pooled = tok_ref[...] + part[me]
    for d in reversed(order):
        copies[d].wait_recv()
        pooled += landed[d - 1]
    pooled = pooled / count.astype(F32)
    everyone[mine] = pooled

    offsets = [(dx, dy) for dx in range(side) for dy in range(side) if dx or dy]
    reach = lambda o: min(o[0], side - o[0]) + min(o[1], side - o[1])
    offsets = sorted(offsets, key=lambda o: -reach(o))
    sends = []
    for i, (dx, dy) in enumerate(offsets):
        copy = pltpu.make_async_remote_copy(
            src_ref=everyone.at[mine],
            dst_ref=everyone.at[mine],
            send_sem=ag_send.at[i],
            recv_sem=ag_recv.at[i],
            device_id={"dp": at(dx, dy)},
        )
        copy.start()
        sends.append(copy)
    relays = [
        pltpu.make_async_remote_copy(
            src_ref=everyone.at[mine],
            dst_ref=everyone.at[mine],
            send_sem=relay_send.at[len(offsets)],
            recv_sem=relay_recv.at[len(offsets)],
            device_id={"dp": partner},
        )
    ]
    relays[0].start()

    lane = lax.broadcasted_iota(jnp.int32, (slots, 128), 1)
    slot = lax.broadcasted_iota(jnp.int32, (slots, 128), 0)
    square = jnp.sum(pooled * pooled, axis=1, keepdims=True)
    square = jnp.sum(jnp.where(lane == slot, square, 0.0), axis=0, keepdims=True)
    square_part[...] = square
    copies_sq = {}
    for d in order:
        copies_sq[d] = pltpu.make_async_remote_copy(
            src_ref=square_part,
            dst_ref=square_landed.at[d - 1],
            send_sem=sq_send.at[d - 1],
            recv_sem=sq_recv.at[d - 1],
            device_id={"mp": (me + d) % mp},
        )
        copies_sq[d].start()
    for d in reversed(order):
        copies_sq[d].wait_recv()
        square += square_landed[d - 1]
    squares[mine] = square

    def share_square(d):
        return pltpu.make_async_remote_copy(
            src_ref=squares.at[mine],
            dst_ref=squares.at[mine],
            send_sem=all_send.at[d - 1],
            recv_sem=all_recv.at[d - 1],
            device_id={"dp": (mine + d) % dp},
        )

    def start_square(d, carry):
        share_square(d).start()
        return carry

    lax.fori_loop(1, dp, start_square, 0)

    for i in reversed(range(len(offsets))):
        dx, dy = offsets[i]
        sends[i].wait_recv()
        source = at(-dx, -dy)
        copy = pltpu.make_async_remote_copy(
            src_ref=everyone.at[source],
            dst_ref=everyone.at[source],
            send_sem=relay_send.at[i],
            recv_sem=relay_recv.at[i],
            device_id={"dp": partner},
        )
        copy.start()
        relays.append(copy)

    total = dp * slots
    classes = proto_ref.shape[0]
    named = episode_v[...] * WAYS + class_v[...]
    named = jnp.where(flag_v[...] == 0, named, -1).reshape(1, total)
    kind = lax.broadcasted_iota(jnp.int32, (classes, total), 0)
    select = jnp.where(kind == named, 1.0, 0.0).astype(BF16)

    def wait_square(d, carry):
        share_square(d).wait_recv()
        return carry

    lax.fori_loop(1, dp, wait_square, 0)
    spread = jnp.where(
        lax.broadcasted_iota(jnp.int32, (dp, slots, 128), 2)
        == lax.broadcasted_iota(jnp.int32, (dp, slots, 128), 1),
        squares[...],
        0.0,
    )
    mean = jnp.sum(spread, axis=2, keepdims=True) * (1.0 / width)
    weight = lax.rsqrt(mean + 1e-06)
    for copy in relays:
        copy.wait_recv()
    scaled = (everyone[...] * weight).reshape(total, share)
    high, low = split(scaled)
    sums = dot(select, high) + dot(select, low)
    own_mean = jnp.sum(
        jnp.where(lane == slot, jnp.broadcast_to(square, (slots, 128)), 0.0), axis=1, keepdims=True
    ) * (1.0 / width)
    own_weight = lax.rsqrt(own_mean + 1e-06)
    own_high, own_low = split(pooled * own_weight)
    sums_high, sums_low = split(sums)
    square_high, square_low = split(sums * sums)
    own = jnp.concatenate([own_high, own_low], axis=0)
    cross = dot_nt(own, sums_high)
    cross = cross[:slots] + cross[slots:] + dot_nt(own, sums_low)[:slots]
    ones = jnp.ones((2 * slots, share), BF16)
    norms = (dot_nt(ones, square_high) + dot_nt(ones, square_low))[:slots]
    mixed = jnp.concatenate([cross, norms], axis=0)
    final_part[...] = mixed
    copies_fin = {}
    for d in order:
        copies_fin[d] = pltpu.make_async_remote_copy(
            src_ref=final_part,
            dst_ref=final_landed.at[d - 1],
            send_sem=fin_send.at[d - 1],
            recv_sem=fin_recv.at[d - 1],
            device_id={"mp": (me + d) % mp},
        )
        copies_fin[d].start()
    for d in reversed(order):
        copies_fin[d].wait_recv()
        mixed += final_landed[d - 1]
    class_mean = mixed[slots : slots + 1] * (1.0 / width)
    class_scale = lax.rsqrt(class_mean + 1e-06)
    diagonal = lax.broadcasted_iota(jnp.int32, (classes, classes), 0) == lax.broadcasted_iota(
        jnp.int32, (classes, classes), 1
    )
    column = jnp.sum(jnp.where(diagonal, class_scale, 0.0), axis=1, keepdims=True)
    proto_ref[...] = sums * column
    own_square = own_mean * own_weight * own_weight
    distance = (own_square + class_mean * class_scale * class_scale) * width - 2.0 * (
        mixed[:slots] * class_scale
    )
    episode = jnp.zeros((slots, 1), jnp.int32)
    asked = jnp.zeros((slots, 1), jnp.int32)
    for s in range(slots):
        episode = jnp.where(row == s, episode_s[mine * slots + s], episode)
        asked = jnp.where(row == s, flag_s[mine * slots + s], asked)
    picked = jnp.zeros((slots, WAYS), F32)
    for e in range(classes // WAYS):
        picked = jnp.where(episode == e, distance[:, e * WAYS : (e + 1) * WAYS], picked)
    logits = picked * (-1.0 / math.sqrt(width))
    shifted = logits - jnp.max(logits, axis=1, keepdims=True)
    result = shifted - jnp.log(jnp.sum(jnp.exp(shifted), axis=1, keepdims=True))
    log_ref[...] = jnp.where(asked == 1, result, 0.0)

    for d in order:
        copies[d].wait_send()
        copies_sq[d].wait_send()
        copies_fin[d].wait_send()
    for copy in sends + relays:
        copy.wait_send()

    def drain(d, carry):
        share_square(d).wait_send()
        return carry

    lax.fori_loop(1, dp, drain, 0)


def exchange(attended, token_sums, w_out, seq_lengths, episode_ids, class_ids, query_flags):
    slots, share = token_sums.shape
    mp, dp = lax.axis_size("mp"), lax.axis_size("dp")
    total = episode_ids.shape[0]
    classes = max(1, total // (2 * WAYS)) * WAYS
    smem = pl.BlockSpec(memory_space=pltpu.SMEM)
    vmem = pl.BlockSpec(memory_space=pltpu.VMEM)
    dma = lambda n: pltpu.SemaphoreType.DMA((n,))
    chips = dp // 2
    return pl.pallas_call(
        exchange_kernel,
        out_shape=(
            jax.ShapeDtypeStruct((slots, WAYS), F32),
            jax.ShapeDtypeStruct((classes, share), F32),
        ),
        in_specs=[smem] * 3 + [vmem] * 6,
        out_specs=(vmem, vmem),
        scratch_shapes=[
            pltpu.VMEM((mp, slots, share), F32),
            pltpu.VMEM((mp - 1, slots, share), F32),
            pltpu.VMEM((dp, slots, share), F32),
            pltpu.VMEM((1, 128), F32),
            pltpu.VMEM((mp - 1, 1, 128), F32),
            pltpu.VMEM((dp, 1, 128), F32),
            pltpu.VMEM((2 * slots, 128), F32),
            pltpu.VMEM((mp - 1, 2 * slots, 128), F32),
            dma(mp - 1),
            dma(mp - 1),
            dma(mp - 1),
            dma(mp - 1),
            dma(chips - 1),
            dma(chips - 1),
            dma(chips),
            dma(chips),
            dma(dp - 1),
            dma(dp - 1),
            dma(mp - 1),
            dma(mp - 1),
        ],
        compiler_params=pltpu.CompilerParams(
            collective_id=0, has_side_effects=True, vmem_limit_bytes=32 * 2**20
        ),
        name="exchange",
    )(
        seq_lengths,
        episode_ids,
        query_flags,
        episode_ids,
        class_ids,
        query_flags,
        attended,
        token_sums,
        w_out,
    )


def per_device(
    tokens,
    norm_gain,
    w_query,
    w_key,
    w_value,
    w_out,
    seq_starts,
    seq_lengths,
    episode_ids,
    class_ids,
    query_flags,
):
    attended, token_sums = local_part(
        tokens, norm_gain, w_query, w_key, w_value, seq_starts, seq_lengths
    )
    return exchange(
        attended, token_sums, w_out, seq_lengths, episode_ids, class_ids, query_flags
    )


def solution(mesh):
    placed = (
        P("dp", None),
        P(),
        P(None, "mp"),
        P(None, "mp"),
        P(None, "mp"),
        P("mp", None),
        P("dp"),
        P("dp"),
        P(),
        P(),
        P(),
    )
    return jax.shard_map(
        per_device,
        mesh=mesh,
        in_specs=placed,
        out_specs=(P("dp", None), P(None, "mp")),
        check_vma=False,
    )
```

```python
import functools
import math

import jax
import jax.numpy as jnp
import numpy as np
from jax import lax
from jax.experimental import pallas as pl
from jax.experimental.pallas import tpu as pltpu
from jax.sharding import PartitionSpec as P

HEAD_DIM = 128
WAYS = 32
ROPE_BASE = 500000.0
LONGEST = 640
STEPS = 8
AHEAD = 3
TILE = 128
ONES = 16
EARLY = 4
SHORTEST = 128
FAR = -(2.0**100)
F32 = jnp.float32
BF16 = jnp.bfloat16


def rope_tables(rows, block):
    half = HEAD_DIM // 2
    frequency = ROPE_BASE ** (-(np.arange(half, dtype=np.float64) * 2.0 / HEAD_DIM))
    frequency = np.concatenate([frequency, frequency])[None, :]
    sign = np.where(np.arange(HEAD_DIM) < half, -1.0, 1.0)[None, :]
    fine = np.arange(block, dtype=np.float64)[:, None] * frequency
    coarse = np.arange(0, rows, block, dtype=np.float64)[:, None] * frequency
    fine_table = np.stack([np.cos(fine), np.sin(fine)])
    coarse_table = np.stack(
        [np.cos(coarse), np.sin(coarse), sign * np.cos(coarse), sign * np.sin(coarse)]
    )
    return fine_table.astype(np.float32), coarse_table.astype(np.float32)


def dot(a, b):
    return jnp.dot(a, b, preferred_element_type=F32)


def dot_nt(a, b):
    return lax.dot_general(a, b, (((1,), (1,)), ((), ())), preferred_element_type=F32)


def split(a):
    high = a.astype(BF16)
    return high, (a - high.astype(F32)).astype(BF16)


def fold(a):
    half = a.shape[1] // 2
    return jnp.concatenate([a[:, :half], a[:, half:]], axis=0)


def whole_kernel(
    starts_h,
    lengths_h,
    episode_h,
    class_h,
    flag_h,
    gain_h,
    fine_h,
    coarse_h,
    x_h,
    wq_h,
    wk_h,
    wv_h,
    wo_h,
    log_ref,
    proto_ref,
    starts,
    lengths,
    episode_s,
    flag_s,
    episode_v,
    class_v,
    flag_v,
    gain,
    fine,
    coarse,
    x_v,
    w_v,
    wo_v,
    acc,
    squares,
    member,
    qs,
    ks,
    vt,
    ot,
    part,
    landed,
    everyone,
    square_part,
    square_landed,
    row_squares,
    final_part,
    final_landed,
    small_sem,
    x_sem,
    wq_sem,
    wk_sem,
    wv_sem,
    late_sem,
    wo_sem,
    rs_send,
    rs_recv,
    sq_send,
    sq_recv,
    ag_send,
    ag_recv,
    relay_send,
    relay_recv,
    all_send,
    all_recv,
    fin_send,
    fin_recv,
):
    mp = lax.axis_size("mp")
    dp = lax.axis_size("dp")
    me = lax.axis_index("mp")
    mine = lax.axis_index("dp")
    rows, width = x_v.shape
    slots = starts.shape[0]
    heads = wq_h.shape[1] // HEAD_DIM
    depth = width // STEPS
    tiles = rows // TILE
    share = width // mp
    late = slots - EARLY
    cut = rows - late * SHORTEST
    late_from = EARLY * SHORTEST
    block = 512

    smalls = [
        pltpu.make_async_copy(source, target, small_sem.at[i])
        for i, (source, target) in enumerate(
            [
                (gain_h, gain),
                (starts_h, starts),
                (lengths_h, lengths),
                (fine_h, fine),
                (coarse_h, coarse),
                (episode_h, episode_s),
                (flag_h, flag_s),
                (episode_h, episode_v),
                (class_h, class_v),
                (flag_h, flag_v),
            ]
        )
    ]

    def chunk_copies(c):
        at = pl.ds(c * depth, depth)
        q, k = heads * HEAD_DIM, HEAD_DIM
        return [
            pltpu.make_async_copy(
                x_h.at[pl.ds(0, cut), at], x_v.at[pl.ds(0, cut), at], x_sem.at[c]
            ),
            pltpu.make_async_copy(wq_h.at[at, :], w_v.at[at, pl.ds(0, q)], wq_sem.at[c]),
            pltpu.make_async_copy(wk_h.at[at, :], w_v.at[at, pl.ds(q, k)], wk_sem.at[c]),
            pltpu.make_async_copy(wv_h.at[at, :], w_v.at[at, pl.ds(q + k, k)], wv_sem.at[c]),
        ]

    smalls[0].start()
    for copy in chunk_copies(0):
        copy.start()
    for copy in smalls[1:]:
        copy.start()
    for c in range(1, AHEAD):
        for copy in chunk_copies(c):
            copy.start()
    late_copy = pltpu.make_async_copy(
        x_h.at[pl.ds(cut, rows - cut), :], x_v.at[pl.ds(cut, rows - cut), :], late_sem.at[0]
    )
    wo_copy = pltpu.make_async_copy(wo_h, wo_v, wo_sem.at[0])

    barrier = pltpu.get_barrier_semaphore()
    for d in range(1, mp):
        pl.semaphore_signal(barrier, inc=1, device_id={"mp": (me + d) % mp})

    def greet(d, carry):
        pl.semaphore_signal(barrier, inc=1, device_id={"dp": (mine + d) % dp})
        return carry

    lax.fori_loop(1, dp, greet, 0)

    def project(first, c, fresh):
        at = pl.ds(first, block)
        deep = pl.ds(c * depth, depth)
        x = x_v[at, deep]
        wide = x.astype(F32)
        wide = wide * wide
        total = wide[:, 0:128]
        for i in range(1, depth // 128):
            total += wide[:, i * 128 : (i + 1) * 128]
        value = dot(x * gain[deep].reshape(1, depth), w_v[deep, :])
        if fresh:
            squares[at, :] = total
            acc[at, :] = value
        else:
            squares[at, :] += total
            acc[at, :] += value

    scale = math.log2(math.e) / math.sqrt(HEAD_DIM)

    def row_scale_of(at):
        return lax.rsqrt(jnp.sum(squares[at, :], axis=1, keepdims=True) * (1.0 / width) + 1e-05)

    def slot_bounds(shape, axis):
        index = lax.broadcasted_iota(jnp.int32, shape, axis)
        first = jnp.full(shape, rows, jnp.int32)
        last = jnp.zeros(shape, jnp.int32)
        for s in range(slots):
            first = jnp.where(index == s, starts[s], first)
            last = jnp.where(index == s, starts[s] + lengths[s], last)
        return first, last

    def prepare(i):
        first, last = slot_bounds((1, 128), 1)
        fine_cos, fine_sin = fine[0], fine[1]
        for h in range(TILE // 64):
            low = i * TILE + h * 64
            at = pl.ds(low, 64)
            row_scale = row_scale_of(at)
            b = low // 64
            cos_a, sin_a = coarse[0, b : b + 1, :], coarse[1, b : b + 1, :]
            cos_s, sin_s = coarse[2, b : b + 1, :], coarse[3, b : b + 1, :]
            cosine = (cos_a * fine_cos - sin_a * fine_sin) * row_scale
            sine = (sin_s * fine_cos + cos_s * fine_sin) * row_scale
            token = low + lax.broadcasted_iota(jnp.int32, (64, 128), 0)
            inside = (token >= first) & (token < last)
            q_mark = jnp.where(inside, 1.0, 0.0).astype(BF16)
            k_mark = jnp.where(inside, 0.0, FAR).astype(BF16)
            for n in range(heads):
                v = acc[at, n * 128 : (n + 1) * 128]
                v = v * cosine + pltpu.roll(v, 64, 1) * sine
                to = pl.ds(n * TILE + h * 64, 64)
                qs[i, to, 0:128] = v.astype(BF16)
                qs[i, to, 128:256] = q_mark
            v = acc[at, heads * 128 : (heads + 1) * 128] * scale
            v = v * cosine + pltpu.roll(v, 64, 1) * sine
            ks[at, 0:128] = v.astype(BF16)
            ks[at, 128:256] = k_mark
        at = pl.ds(i * TILE, TILE)
        v = acc[at, (heads + 1) * 128 : (heads + 2) * 128] * row_scale_of(at)
        vt[0:128, at] = v.T.astype(BF16)
        vt[128 : 128 + ONES, at] = jnp.ones((ONES, TILE), BF16)

    def attend(i):
        key = lax.broadcasted_iota(jnp.int32, (TILE, heads * TILE), 0)
        query = lax.broadcasted_iota(jnp.int32, (TILE, heads * TILE), 1) % TILE
        begin = max(0, i * TILE - LONGEST)
        before = i * TILE - begin
        s = dot_nt(ks[begin : (i + 1) * TILE, :], qs[i])
        own = jnp.where(key <= query, s[before:], FAR)
        peak = jnp.max(own, axis=0, keepdims=True)
        if before:
            peak = jnp.maximum(peak, jnp.max(s[:before], axis=0, keepdims=True))
        e = jnp.exp2(own - peak).astype(BF16)
        if before:
            e = jnp.concatenate([jnp.exp2(s[:before] - peak).astype(BF16), e], axis=0)
        o = dot(vt[:, begin : (i + 1) * TILE], e)
        o = (o[0:128] / o[128:129]).astype(BF16)
        for n in range(heads):
            ot[n * 128 : (n + 1) * 128, i * TILE : (i + 1) * TILE] = o[:, n * TILE : (n + 1) * TILE]

    def head_part(group):
        span = slice(0, cut) if group == 0 else slice(late_from, rows)
        pick = slice(0, EARLY) if group == 0 else slice(EARLY, slots)
        high, low = split(dot_nt(member[:, span], ot[:, span])[pick])
        stacked = jnp.concatenate([high, low], axis=0)
        for r in range(mp):
            both = dot(stacked, wo_v[:, r * share : (r + 1) * share])
            n = both.shape[0] // 2
            part[group, r] = fold(both[:n] + both[n:])

    def token_part(group):
        span = slice(0, cut) if group == 0 else slice(late_from, rows)
        pick = slice(0, EARLY) if group == 0 else slice(EARLY, slots)
        own = pl.ds(pl.multiple_of(me * share, share), share)
        return fold(dot(member[:, span], x_v[span, own])[pick])

    order = sorted(range(1, mp), key=lambda d: -min(d, mp - d))

    def reduce_copies(group):
        return {
            d: pltpu.make_async_remote_copy(
                src_ref=part.at[group, (me + d) % mp],
                dst_ref=landed.at[group, d - 1],
                send_sem=rs_send.at[group, d - 1],
                recv_sem=rs_recv.at[group, d - 1],
                device_id={"mp": (me + d) % mp},
            )
            for d in order
        }

    def reduced(group, copies, tokens_sum):
        value = tokens_sum + part[group, me]
        for d in reversed(order):
            copies[d].wait_recv()
            value += landed[group, d - 1]
        size = value.shape[0]
        row = lax.broadcasted_iota(jnp.int32, (size, 1), 0)
        count = jnp.ones((size, 1), jnp.int32)
        for s in range(size):
            count = jnp.where(row == s, lengths[group * EARLY + s % (size // 2)], count)
        return value / count.astype(F32)

    side = int(math.isqrt(dp // 2))
    x, y, core = mine // (2 * side), (mine // 2) % side, mine % 2
    partner = mine + 1 - 2 * core

    def at_offset(dx, dy):
        return (((x + dx + side) % side) * side + (y + dy + side) % side) * 2 + core

    reach = lambda o: min(o[0], side - o[0]) + min(o[1], side - o[1])
    offsets = [(dx, dy) for dx in range(side) for dy in range(side) if dx or dy]
    offsets = sorted(offsets, key=lambda o: -reach(o))

    def gather_copy(group, i):
        return pltpu.make_async_remote_copy(
            src_ref=everyone.at[group, mine],
            dst_ref=everyone.at[group, mine],
            send_sem=ag_send.at[group, i],
            recv_sem=ag_recv.at[group, i],
            device_id={"dp": at_offset(*offsets[i])},
        )

    def relay_copy(group, i):
        source = mine if i == len(offsets) else at_offset(-offsets[i][0], -offsets[i][1])
        return pltpu.make_async_remote_copy(
            src_ref=everyone.at[group, source],
            dst_ref=everyone.at[group, source],
            send_sem=relay_send.at[group, i],
            recv_sem=relay_recv.at[group, i],
            device_id={"dp": partner},
        )

    def gather(group):
        for i in range(len(offsets)):
            gather_copy(group, i).start()
        relay_copy(group, len(offsets)).start()

    def relay(group):
        for i in reversed(range(len(offsets))):
            gather_copy(group, i).wait_recv()
            relay_copy(group, i).start()

    for c in range(STEPS):
        if c == 0:
            smalls[0].wait()
        for copy in chunk_copies(c):
            copy.wait()
        if c + AHEAD < STEPS:
            for copy in chunk_copies(c + AHEAD):
                copy.start()
        if c + AHEAD == STEPS:
            late_copy.start()
        if c + AHEAD == STEPS + 1:
            wo_copy.start()
        for first in range(0, cut, block):
            project(first, c, c == 0)
    for copy in smalls[1:]:
        copy.wait()
    token = lax.broadcasted_iota(jnp.int32, (ONES, rows), 1)
    first, last = slot_bounds((ONES, rows), 0)
    member[...] = jnp.where((token >= first) & (token < last), 1.0, 0.0).astype(BF16)
    for i in range(cut // TILE):
        prepare(i)
    for i in range(cut // TILE):
        attend(i)
    wo_copy.wait()
    head_part(0)
    pl.semaphore_wait(barrier, mp - 1 + dp - 1)
    reduce_early = reduce_copies(0)
    for d in order:
        reduce_early[d].start()

    late_copy.wait()
    for c in range(STEPS):
        for first in range(cut, rows, block):
            project(first, c, c == 0)
    tokens_early = token_part(0)
    pooled_early = reduced(0, reduce_early, tokens_early)
    everyone[0, mine] = pooled_early
    gather(0)

    for i in range(cut // TILE, tiles):
        prepare(i)
    for i in range(cut // TILE, tiles):
        attend(i)
    head_part(1)
    reduce_late = reduce_copies(1)
    for d in order:
        reduce_late[d].start()
    tokens_late = token_part(1)
    relay(0)
    pooled_late = reduced(1, reduce_late, tokens_late)
    everyone[1, mine] = pooled_late
    gather(1)

    lane = lax.broadcasted_iota(jnp.int32, (slots, 128), 1)
    slot = lax.broadcasted_iota(jnp.int32, (slots, 128), 0)
    parts = []
    for group, value in enumerate((pooled_early, pooled_late)):
        total = jnp.sum(value * value, axis=1, keepdims=True)
        parts.append(jnp.where(lane % EARLY == slot % EARLY, total, 0.0))
    parts = jnp.where(lane < EARLY, parts[0], jnp.where(lane < slots, parts[1], 0.0))
    square = jnp.sum(parts, axis=0, keepdims=True)
    square_part[...] = square
    copies_sq = {}
    for d in order:
        copies_sq[d] = pltpu.make_async_remote_copy(
            src_ref=square_part,
            dst_ref=square_landed.at[d - 1],
            send_sem=sq_send.at[d - 1],
            recv_sem=sq_recv.at[d - 1],
            device_id={"mp": (me + d) % mp},
        )
        copies_sq[d].start()
    for d in reversed(order):
        copies_sq[d].wait_recv()
        square += square_landed[d - 1]
    row_squares[mine] = square

    def share_square(d):
        return pltpu.make_async_remote_copy(
            src_ref=row_squares.at[mine],
            dst_ref=row_squares.at[mine],
            send_sem=all_send.at[d - 1],
            recv_sem=all_recv.at[d - 1],
            device_id={"dp": (mine + d) % dp},
        )

    def start_square(d, carry):
        share_square(d).start()
        return carry

    lax.fori_loop(1, dp, start_square, 0)
    relay(1)

    total = dp * slots
    classes = proto_ref.shape[0]
    named = episode_v[...] * WAYS + class_v[...]
    named = jnp.where(flag_v[...] == 0, named, -1).reshape(1, total)
    kind = lax.broadcasted_iota(jnp.int32, (classes, total), 0)
    select = jnp.where(kind == named, 1.0, 0.0).astype(BF16)

    def wait_square(d, carry):
        share_square(d).wait_recv()
        return carry

    lax.fori_loop(1, dp, wait_square, 0)
    spread = jnp.where(
        lax.broadcasted_iota(jnp.int32, (dp, slots, 128), 2)
        == lax.broadcasted_iota(jnp.int32, (dp, slots, 128), 1),
        row_squares[...],
        0.0,
    )
    weight = lax.rsqrt(jnp.sum(spread, axis=2, keepdims=True) * (1.0 / width) + 1e-06)
    for group in range(2):
        for i in range(len(offsets) + 1):
            relay_copy(group, i).wait_recv()

    def unfold(early, late):
        axis = early.ndim - 2
        a = [lax.slice_in_dim(early, h * EARLY, (h + 1) * EARLY, axis=axis) for h in range(2)]
        b = [lax.slice_in_dim(late, h * EARLY, (h + 1) * EARLY, axis=axis) for h in range(2)]
        return jnp.concatenate(
            [jnp.concatenate([a[h], b[h]], axis=axis) for h in range(2)], axis=axis + 1
        )

    scaled = (unfold(everyone[0], everyone[1]) * weight).reshape(total, share)
    high, low = split(scaled)
    sums = dot(select, high) + dot(select, low)
    own_mean = jnp.sum(
        jnp.where(lane == slot, jnp.broadcast_to(square, (slots, 128)), 0.0), axis=1, keepdims=True
    ) * (1.0 / width)
    own_weight = lax.rsqrt(own_mean + 1e-06)
    own_high, own_low = split(unfold(pooled_early, pooled_late) * own_weight)
    sums_high, sums_low = split(sums)
    square_high, square_low = split(sums * sums)
    own = jnp.concatenate([own_high, own_low], axis=0)
    cross = dot_nt(own, sums_high)
    cross = cross[:slots] + cross[slots:] + dot_nt(own, sums_low)[:slots]
    ones = jnp.ones((2 * slots, share), BF16)
    norms = (dot_nt(ones, square_high) + dot_nt(ones, square_low))[:slots]
    mixed = jnp.concatenate([cross, norms], axis=0)
    final_part[...] = mixed
    copies_fin = {}
    for d in order:
        copies_fin[d] = pltpu.make_async_remote_copy(
            src_ref=final_part,
            dst_ref=final_landed.at[d - 1],
            send_sem=fin_send.at[d - 1],
            recv_sem=fin_recv.at[d - 1],
            device_id={"mp": (me + d) % mp},
        )
        copies_fin[d].start()
    for d in reversed(order):
        copies_fin[d].wait_recv()
        mixed += final_landed[d - 1]
    class_mean = mixed[slots : slots + 1] * (1.0 / width)
    class_scale = lax.rsqrt(class_mean + 1e-06)
    diagonal = lax.broadcasted_iota(jnp.int32, (classes, classes), 0) == lax.broadcasted_iota(
        jnp.int32, (classes, classes), 1
    )
    column = jnp.sum(jnp.where(diagonal, class_scale, 0.0), axis=1, keepdims=True)
    proto_ref[...] = sums * column
    own_square = own_mean * own_weight * own_weight
    distance = (own_square + class_mean * class_scale * class_scale) * width - 2.0 * (
        mixed[:slots] * class_scale
    )
    row = lax.broadcasted_iota(jnp.int32, (slots, 1), 0)
    episode = jnp.zeros((slots, 1), jnp.int32)
    asked = jnp.zeros((slots, 1), jnp.int32)
    for s in range(slots):
        episode = jnp.where(row == s, episode_s[mine * slots + s], episode)
        asked = jnp.where(row == s, flag_s[mine * slots + s], asked)
    picked = jnp.zeros((slots, WAYS), F32)
    for e in range(classes // WAYS):
        picked = jnp.where(episode == e, distance[:, e * WAYS : (e + 1) * WAYS], picked)
    logits = picked * (-1.0 / math.sqrt(width))
    shifted = logits - jnp.max(logits, axis=1, keepdims=True)
    result = shifted - jnp.log(jnp.sum(jnp.exp(shifted), axis=1, keepdims=True))
    log_ref[...] = jnp.where(asked == 1, result, 0.0)

    for d in order:
        reduce_early[d].wait_send()
        reduce_late[d].wait_send()
        copies_sq[d].wait_send()
        copies_fin[d].wait_send()
    for group in range(2):
        for i in range(len(offsets)):
            gather_copy(group, i).wait_send()
        for i in range(len(offsets) + 1):
            relay_copy(group, i).wait_send()

    def drain(d, carry):
        share_square(d).wait_send()
        return carry

    lax.fori_loop(1, dp, drain, 0)


def per_device(
    tokens,
    norm_gain,
    w_query,
    w_key,
    w_value,
    w_out,
    seq_starts,
    seq_lengths,
    episode_ids,
    class_ids,
    query_flags,
):
    rows, width = tokens.shape
    slots = seq_starts.shape[0]
    inner = w_query.shape[1]
    heads = inner // HEAD_DIM
    columns = inner + w_key.shape[1] + w_value.shape[1]
    mp, dp = lax.axis_size("mp"), lax.axis_size("dp")
    share = width // mp
    tiles = rows // TILE
    total = episode_ids.shape[0]
    classes = max(1, total // (2 * WAYS)) * WAYS
    chips = dp // 2
    fine, coarse = rope_tables(rows, 64)
    hbm = pl.BlockSpec(memory_space=pltpu.HBM)
    vmem = pl.BlockSpec(memory_space=pltpu.VMEM)
    dma = lambda *n: pltpu.SemaphoreType.DMA(n)
    ints = lambda n: pltpu.SMEM((n,), jnp.int32)
    return pl.pallas_call(
        whole_kernel,
        out_shape=(
            jax.ShapeDtypeStruct((slots, WAYS), F32),
            jax.ShapeDtypeStruct((classes, share), F32),
        ),
        in_specs=[hbm] * 13,
        out_specs=(vmem, vmem),
        scratch_shapes=[
            ints(slots),
            ints(slots),
            ints(total),
            ints(total),
            pltpu.VMEM((total,), jnp.int32),
            pltpu.VMEM((total,), jnp.int32),
            pltpu.VMEM((total,), jnp.int32),
            pltpu.VMEM((width,), BF16),
            pltpu.VMEM(fine.shape, F32),
            pltpu.VMEM(coarse.shape, F32),
            pltpu.VMEM((rows, width), BF16),
            pltpu.VMEM((width, columns), BF16),
            pltpu.VMEM((inner, width), BF16),
            pltpu.VMEM((rows, columns), F32),
            pltpu.VMEM((rows, 128), F32),
            pltpu.VMEM((ONES, rows), BF16),
            pltpu.VMEM((tiles, heads * TILE, 256), BF16),
            pltpu.VMEM((rows, 256), BF16),
            pltpu.VMEM((128 + ONES, rows), BF16),
            pltpu.VMEM((inner, rows), BF16),
            pltpu.VMEM((2, mp, slots, share // 2), F32),
            pltpu.VMEM((2, mp - 1, slots, share // 2), F32),
            pltpu.VMEM((2, dp, slots, share // 2), F32),
            pltpu.VMEM((1, 128), F32),
            pltpu.VMEM((mp - 1, 1, 128), F32),
            pltpu.VMEM((dp, 1, 128), F32),
            pltpu.VMEM((2 * slots, 128), F32),
            pltpu.VMEM((mp - 1, 2 * slots, 128), F32),
            dma(10),
            dma(STEPS),
            dma(STEPS),
            dma(STEPS),
            dma(STEPS),
            dma(1),
            dma(1),
            dma(2, mp - 1),
            dma(2, mp - 1),
            dma(mp - 1),
            dma(mp - 1),
            dma(2, chips - 1),
            dma(2, chips - 1),
            dma(2, chips),
            dma(2, chips),
            dma(dp - 1),
            dma(dp - 1),
            dma(mp - 1),
            dma(mp - 1),
        ],
        compiler_params=pltpu.CompilerParams(
            collective_id=0, has_side_effects=True, vmem_limit_bytes=60 * 2**20
        ),
        name="whole",
    )(
        seq_starts,
        seq_lengths,
        episode_ids,
        class_ids,
        query_flags,
        norm_gain,
        jnp.asarray(fine),
        jnp.asarray(coarse),
        tokens,
        w_query,
        w_key,
        w_value,
        w_out,
    )


def solution(mesh):
    placed = (
        P("dp", None),
        P(),
        P(None, "mp"),
        P(None, "mp"),
        P(None, "mp"),
        P("mp", None),
        P("dp"),
        P("dp"),
        P(),
        P(),
        P(),
    )
    return jax.shard_map(
        per_device,
        mesh=mesh,
        in_specs=placed,
        out_specs=(P("dp", None), P(None, "mp")),
        check_vma=False,
    )
```

```python
import functools
import math

import jax
import jax.numpy as jnp
import numpy as np
from jax import lax
from jax.experimental import pallas as pl
from jax.experimental.pallas import tpu as pltpu
from jax.sharding import PartitionSpec as P

HEAD_DIM = 128
WAYS = 32
ROPE_BASE = 500000.0
LONGEST = 640
STEPS = 8
AHEAD = 3
TILE = 128
ONES = 16
EARLY = 4
PIECES = 2
BLOCK = 512
SHORTEST = 128
FAR = -(2.0**100)
F32 = jnp.float32
BF16 = jnp.bfloat16


def rope_tables(rows, block):
    half = HEAD_DIM // 2
    frequency = ROPE_BASE ** (-(np.arange(half, dtype=np.float64) * 2.0 / HEAD_DIM))
    frequency = np.concatenate([frequency, frequency])[None, :]
    sign = np.where(np.arange(HEAD_DIM) < half, -1.0, 1.0)[None, :]
    fine = np.arange(block, dtype=np.float64)[:, None] * frequency
    coarse = np.arange(0, rows, block, dtype=np.float64)[:, None] * frequency
    fine_table = np.stack([np.cos(fine), np.sin(fine)])
    coarse_table = np.stack(
        [np.cos(coarse), np.sin(coarse), sign * np.cos(coarse), sign * np.sin(coarse)]
    )
    return fine_table.astype(np.float32), coarse_table.astype(np.float32)


def dot(a, b):
    return jnp.dot(a, b, preferred_element_type=F32)


def dot_nt(a, b):
    return lax.dot_general(a, b, (((1,), (1,)), ((), ())), preferred_element_type=F32)


def split(a):
    high = a.astype(BF16)
    return high, (a - high.astype(F32)).astype(BF16)


def fold(a):
    span = a.shape[1] // PIECES
    return jnp.concatenate([a[:, p * span : (p + 1) * span] for p in range(PIECES)], axis=0)


def unfold(a, before, after):
    axis = a.ndim - 2
    size = a.shape[axis] // PIECES
    pad = lambda n: [jnp.zeros(a.shape[:axis] + (n, a.shape[-1]), a.dtype)] if n else []
    pieces = [
        jnp.concatenate(
            pad(before)
            + [lax.slice_in_dim(a, p * size, (p + 1) * size, axis=axis)]
            + pad(after),
            axis=axis,
        )
        for p in range(PIECES)
    ]
    return jnp.concatenate(pieces, axis=axis + 1)


def whole_kernel(
    starts_h,
    lengths_h,
    episode_h,
    class_h,
    flag_h,
    gain_h,
    fine_h,
    coarse_h,
    x_h,
    wq_h,
    wk_h,
    wv_h,
    wo_h,
    log_ref,
    proto_ref,
    starts,
    lengths,
    episode_s,
    flag_s,
    episode_v,
    class_v,
    flag_v,
    gain,
    fine,
    coarse,
    x_v,
    w_v,
    wo_v,
    acc,
    squares,
    member,
    qt,
    ks,
    vt,
    ot,
    part,
    landed,
    everyone,
    late_part,
    late_landed,
    late_total,
    late_everyone,
    square_part,
    square_landed,
    final_part,
    final_landed,
    small_sem,
    x_sem,
    wq_sem,
    wk_sem,
    wv_sem,
    wo_sem,
    rs_send,
    rs_recv,
    ar_send,
    ar_recv,
    sq_send,
    sq_recv,
    ag_send,
    ag_recv,
    relay_send,
    relay_recv,
    fin_send,
    fin_recv,
):
    mp = lax.axis_size("mp")
    dp = lax.axis_size("dp")
    me = lax.axis_index("mp")
    mine = lax.axis_index("dp")
    rows, width = x_h.shape
    slots = starts.shape[0]
    heads = wq_h.shape[1] // HEAD_DIM
    depth = width // STEPS
    tiles = rows // TILE
    share = width // mp
    late = slots - EARLY
    late_rows = late
    cut = rows - late * SHORTEST
    late_from = EARLY * SHORTEST

    smalls = [
        pltpu.make_async_copy(source, target, small_sem.at[i])
        for i, (source, target) in enumerate(
            [
                (gain_h, gain),
                (starts_h, starts),
                (lengths_h, lengths),
                (fine_h, fine),
                (coarse_h, coarse),
                (episode_h, episode_s),
                (flag_h, flag_s),
                (episode_h, episode_v),
                (class_h, class_v),
                (flag_h, flag_v),
            ]
        )
    ]

    bounds = [(0, depth // 2), (depth // 2, depth // 2)]
    bounds += [(depth, depth)]
    bounds += [(c * depth, 2 * depth) for c in range(2, STEPS, 2)]

    def chunk_copies(c):
        at = pl.ds(*bounds[c])
        q, k = heads * HEAD_DIM, HEAD_DIM
        return [
            pltpu.make_async_copy(
                x_h.at[:, at], x_v.at[:, at], x_sem.at[c]
            ),
            pltpu.make_async_copy(wq_h.at[at, :], w_v.at[at, pl.ds(0, q)], wq_sem.at[c]),
            pltpu.make_async_copy(wk_h.at[at, :], w_v.at[at, pl.ds(q, k)], wk_sem.at[c]),
            pltpu.make_async_copy(wv_h.at[at, :], w_v.at[at, pl.ds(q + k, k)], wv_sem.at[c]),
        ]

    smalls[0].start()
    for copy in chunk_copies(0):
        copy.start()
    for copy in smalls[1:]:
        copy.start()
    for c in range(1, AHEAD):
        for copy in chunk_copies(c):
            copy.start()
    wo_copy = pltpu.make_async_copy(wo_h, wo_v, wo_sem.at[0])

    def lane_squares(x):
        wide = x.astype(F32)
        wide = wide * wide
        total = wide[:, 0:128]
        for i in range(1, x.shape[1] // 128):
            total += wide[:, i * 128 : (i + 1) * 128]
        return total

    def project_chunk(c):
        deep = pl.ds(*bounds[c])
        for first in range(0, rows, BLOCK):
            at = pl.ds(first, BLOCK)
            x = x_v[at, deep]
            value = dot(x * gain[deep].reshape(1, bounds[c][1]), w_v[deep, :])
            if c == 0:
                squares[at, :] = lane_squares(x)
                acc[at, :] = value
            else:
                squares[at, :] += lane_squares(x)
                acc[at, :] += value

    scale = math.log2(math.e) / math.sqrt(HEAD_DIM)

    def row_scale_of(at):
        return lax.rsqrt(jnp.sum(squares[at, :], axis=1, keepdims=True) * (1.0 / width) + 1e-05)

    def slot_bounds(shape, axis):
        index = lax.broadcasted_iota(jnp.int32, shape, axis)
        first = jnp.full(shape, rows, jnp.int32)
        last = jnp.zeros(shape, jnp.int32)
        for s in range(slots):
            first = jnp.where(index == s, starts[s], first)
            last = jnp.where(index == s, starts[s] + lengths[s], last)
        return first, last

    def prepare(i):
        first, last = slot_bounds((1, 128), 1)
        fine_cos, fine_sin = fine[0], fine[1]
        at = pl.ds(i * TILE, TILE)
        row_scale = row_scale_of(at)
        cosines, sines = [], []
        for b in range(i * TILE // 64, (i + 1) * TILE // 64):
            cos_a, sin_a = coarse[0, b : b + 1, :], coarse[1, b : b + 1, :]
            cos_s, sin_s = coarse[2, b : b + 1, :], coarse[3, b : b + 1, :]
            cosines.append(cos_a * fine_cos - sin_a * fine_sin)
            sines.append(sin_s * fine_cos + cos_s * fine_sin)
        cosine = jnp.concatenate(cosines, axis=0) * row_scale
        sine = jnp.concatenate(sines, axis=0) * row_scale
        for n in range(heads):
            v = acc[at, n * 128 : (n + 1) * 128]
            v = v * cosine + pltpu.roll(v, 64, 1) * sine
            qt[i % 3, 0:128, n * TILE : (n + 1) * TILE] = v.T.astype(BF16)
            qt[i % 3, 128 : 128 + ONES, n * TILE : (n + 1) * TILE] = member[:, at]
        v = acc[at, heads * 128 : (heads + 1) * 128] * scale
        v = v * cosine + pltpu.roll(v, 64, 1) * sine
        ks[at, 0:128] = v.astype(BF16)
        token = i * TILE + lax.broadcasted_iota(jnp.int32, (TILE, 128), 0)
        inside = (token >= first) & (token < last)
        ks[at, 128:256] = jnp.where(inside, 0.0, FAR).astype(BF16)
        v = acc[at, (heads + 1) * 128 : (heads + 2) * 128] * row_scale
        vt[0:128, at] = v.T.astype(BF16)
        vt[128 : 128 + ONES, at] = jnp.ones((ONES, TILE), BF16)

    def score(i):
        begin = max(0, i * TILE - LONGEST)
        return dot(ks[begin : (i + 1) * TILE, :], qt[i % 3])

    def mix(i, s):
        key = lax.broadcasted_iota(jnp.int32, (TILE, heads * TILE), 0)
        query = lax.broadcasted_iota(jnp.int32, (TILE, heads * TILE), 1) % TILE
        begin = max(0, i * TILE - LONGEST)
        before = i * TILE - begin
        own = jnp.where(key <= query, s[before:], FAR)
        peak = jnp.max(own, axis=0, keepdims=True)
        if before:
            peak = jnp.maximum(peak, jnp.max(s[:before], axis=0, keepdims=True))
        e = jnp.exp2(own - peak).astype(BF16)
        if before:
            e = jnp.concatenate([jnp.exp2(s[:before] - peak).astype(BF16), e], axis=0)
        o = dot(vt[:, begin : (i + 1) * TILE], e)
        o = (o[0:128] / o[128:129]).astype(BF16)
        for n in range(heads):
            ot[n * 128 : (n + 1) * 128, i * TILE : (i + 1) * TILE] = o[:, n * TILE : (n + 1) * TILE]

    def attend(first, last):
        prepare(first)
        ready = score(first)
        for i in range(first, last):
            now = ready
            if i + 1 < last:
                prepare(i + 1)
                ready = score(i + 1)
            mix(i, now)

    def head_part(span, pick, target):
        high, low = split(dot_nt(member[:, span], ot[:, span])[pick])
        stacked = jnp.concatenate([high, low], axis=0)
        for r in range(mp):
            both = dot(stacked, wo_v[:, r * share : (r + 1) * share])
            n = both.shape[0] // 2
            target[r] = fold(both[:n] + both[n:])

    def divided(value, first, size):
        row = lax.broadcasted_iota(jnp.int32, (value.shape[0], 1), 0)
        count = jnp.ones(row.shape, jnp.int32)
        for s in range(value.shape[0]):
            count = jnp.where(row == s, lengths[first + s % size], count)
        return value / count.astype(F32)

    order = sorted(range(1, mp), key=lambda d: -min(d, mp - d))

    def to_ranks(source, target, send, recv):
        return {
            d: pltpu.make_async_remote_copy(
                src_ref=source(d),
                dst_ref=target.at[d - 1],
                send_sem=send.at[d - 1],
                recv_sem=recv.at[d - 1],
                device_id={"mp": (me + d) % mp},
            )
            for d in order
        }

    side = int(math.isqrt(dp // 2))
    x, y, core = mine // (2 * side), (mine // 2) % side, mine % 2
    partner = mine + 1 - 2 * core

    def at_offset(dx, dy):
        return (((x + dx + side) % side) * side + (y + dy + side) % side) * 2 + core

    reach = lambda o: min(o[0], side - o[0]) + min(o[1], side - o[1])
    offsets = [(dx, dy) for dx in range(side) for dy in range(side) if dx or dy]
    offsets = sorted(offsets, key=lambda o: -reach(o))

    gathered = (everyone, late_everyone)

    def gather_copy(group, i):
        return pltpu.make_async_remote_copy(
            src_ref=gathered[group].at[mine],
            dst_ref=gathered[group].at[mine],
            send_sem=ag_send.at[group, i],
            recv_sem=ag_recv.at[group, i],
            device_id={"dp": at_offset(*offsets[i])},
        )

    def relay_copy(group, i):
        source = mine if i == len(offsets) else at_offset(-offsets[i][0], -offsets[i][1])
        return pltpu.make_async_remote_copy(
            src_ref=gathered[group].at[source],
            dst_ref=gathered[group].at[source],
            send_sem=relay_send.at[group, i],
            recv_sem=relay_recv.at[group, i],
            device_id={"dp": partner},
        )

    def gather(group):
        for i in range(len(offsets)):
            gather_copy(group, i).start()
        relay_copy(group, len(offsets)).start()

    def relay(group):
        for i in reversed(range(len(offsets))):
            gather_copy(group, i).wait_recv()
            relay_copy(group, i).start()

    barrier = pltpu.get_barrier_semaphore()
    for d in range(1, mp):
        pl.semaphore_signal(barrier, inc=1, device_id={"mp": (me + d) % mp})
    for offset in offsets:
        pl.semaphore_signal(barrier, inc=1, device_id={"dp": at_offset(*offset)})
    pl.semaphore_signal(barrier, inc=1, device_id={"dp": partner})
    smalls[0].wait()
    for c in range(len(bounds)):
        for copy in chunk_copies(c):
            copy.wait()
        if c + AHEAD < len(bounds):
            for copy in chunk_copies(c + AHEAD):
                copy.start()
        elif c + AHEAD == len(bounds):
            wo_copy.start()
        project_chunk(c)
    for copy in smalls[1:]:
        copy.wait()
    token = lax.broadcasted_iota(jnp.int32, (ONES, rows), 1)
    first, last = slot_bounds((ONES, rows), 0)
    member[...] = jnp.where((token >= first) & (token < last), 1.0, 0.0).astype(BF16)
    qt[:, 128 + ONES :, :] = jnp.zeros((3, 128 - ONES, heads * TILE), BF16)
    attend(0, cut // TILE)
    wo_copy.wait()
    head_part(slice(0, cut), slice(0, EARLY), part)
    pl.semaphore_wait(barrier, mp - 1 + len(offsets) + 1)
    reduce_early = to_ranks(lambda d: part.at[(me + d) % mp], landed, rs_send, rs_recv)
    for d in order:
        reduce_early[d].start()

    own_features = pl.ds(pl.multiple_of(me * share, share), share)
    pooled = fold(dot(member[:, :cut], x_v[:cut, own_features])[:EARLY])
    attend(cut // TILE, tiles)
    head_part(slice(late_from, rows), slice(EARLY, slots), late_part)
    reduce_late = to_ranks(lambda d: late_part, late_landed, ar_send, ar_recv)
    for d in order:
        reduce_late[d].start()

    pooled += part[me]
    for d in reversed(order):
        reduce_early[d].wait_recv()
        pooled += landed[d - 1]
    pooled = divided(pooled, 0, EARLY)
    everyone[mine] = pooled
    gather(0)
    late_tokens = dot(member[:, late_from:], x_v[late_from:, :])[EARLY:slots]
    for r in range(mp):
        late_total[r] = fold(late_tokens[:, r * share : (r + 1) * share]) + late_part[r]
    total = dp * slots
    classes = proto_ref.shape[0]
    named = episode_v[...] * WAYS + class_v[...]
    named = jnp.where(flag_v[...] == 0, named, -1).reshape(1, total)
    kind = lax.broadcasted_iota(jnp.int32, (classes, total), 0)
    select = jnp.where(kind == named, 1.0, 0.0).astype(BF16)
    relay(0)
    for i in range(len(offsets) + 1):
        relay_copy(0, i).wait_recv()
    early = unfold(everyone[...], 0, late_rows)
    square = jnp.sum(early * early, axis=2, keepdims=True)
    wide_lane = lax.broadcasted_iota(jnp.int32, (dp, slots, 128), 2)
    wide_slot = lax.broadcasted_iota(jnp.int32, (dp, slots, 128), 1)
    square = jnp.sum(jnp.where(wide_lane == wide_slot, square, 0.0), axis=1)
    square_part[...] = square
    copies_sq = to_ranks(lambda d: square_part, square_landed, sq_send, sq_recv)
    for d in order:
        copies_sq[d].start()
    for d in reversed(order):
        reduce_late[d].wait_recv()
    late_square = jnp.zeros((late_rows * PIECES, 1), F32)
    for r in range(mp):
        value = late_total[r]
        for d in order:
            value += late_landed[d - 1, r]
        value = divided(value, EARLY, late_rows)
        late_total[r] = value
        late_square += jnp.sum(value * value, axis=1, keepdims=True)
    lane = lax.broadcasted_iota(jnp.int32, (slots, 128), 1)
    slot = lax.broadcasted_iota(jnp.int32, (slots, 128), 0)
    late_square = jnp.sum(
        jnp.where(lane % late_rows == slot % late_rows, late_square, 0.0), axis=0, keepdims=True
    )
    late_mean = jnp.sum(
        jnp.where(lane == slot % late_rows, late_square, 0.0), axis=1, keepdims=True
    ) * (1.0 / width)
    late_own = late_total[me] * lax.rsqrt(late_mean + 1e-06)
    late_everyone[mine] = late_own
    gather(1)

    for d in reversed(order):
        copies_sq[d].wait_recv()
        square += square_landed[d - 1]
    square_part_total = square.reshape(dp, 1, 128)
    mean = jnp.sum(
        jnp.where(wide_lane == wide_slot, square_part_total, 0.0), axis=2, keepdims=True
    ) * (1.0 / width)
    high, low = split((early * lax.rsqrt(mean + 1e-06)).reshape(total, share))
    sums = dot(select, high) + dot(select, low)
    own_row = lax.broadcasted_iota(jnp.int32, (dp, 128), 0) == mine
    own_square = jnp.sum(jnp.where(own_row, square, 0.0), axis=0, keepdims=True)
    own_square = jnp.where(slot >= EARLY, late_square, own_square)
    own_mean = jnp.sum(jnp.where(lane == slot, own_square, 0.0), axis=1, keepdims=True) * (
        1.0 / width
    )
    own_weight = lax.rsqrt(own_mean + 1e-06)
    own = unfold(pooled, 0, late_rows) * own_weight + unfold(late_own, EARLY, 0)
    own_high, own_low = split(own)
    own = jnp.concatenate([own_high, own_low], axis=0)
    relay(1)
    for i in range(len(offsets) + 1):
        relay_copy(1, i).wait_recv()
    high, low = split(unfold(late_everyone[...], EARLY, 0).reshape(total, share))
    sums += dot(select, high) + dot(select, low)
    sums_high, sums_low = split(sums)
    diagonal = lax.broadcasted_iota(jnp.int32, (classes, classes), 0) == lax.broadcasted_iota(
        jnp.int32, (classes, classes), 1
    )
    norms = jnp.sum(sums * sums, axis=1, keepdims=True)
    norms = jnp.sum(jnp.where(diagonal, norms, 0.0), axis=0, keepdims=True)
    cross = dot_nt(own, sums_high)
    cross = cross[:slots] + cross[slots:] + dot_nt(own, sums_low)[:slots]
    mixed = jnp.concatenate([cross, jnp.broadcast_to(norms, (slots, classes))], axis=0)
    final_part[...] = mixed
    copies_fin = to_ranks(lambda d: final_part, final_landed, fin_send, fin_recv)
    for d in order:
        copies_fin[d].start()
    for d in reversed(order):
        copies_fin[d].wait_recv()
        mixed += final_landed[d - 1]
    class_mean = mixed[slots : slots + 1] * (1.0 / width)
    class_scale = lax.rsqrt(class_mean + 1e-06)
    column = jnp.sum(jnp.where(diagonal, class_scale, 0.0), axis=1, keepdims=True)
    proto_ref[...] = sums * column
    distance = (
        own_mean * own_weight * own_weight + class_mean * class_scale * class_scale
    ) * width - 2.0 * (mixed[:slots] * class_scale)
    row = lax.broadcasted_iota(jnp.int32, (slots, 1), 0)
    episode = jnp.zeros((slots, 1), jnp.int32)
    asked = jnp.zeros((slots, 1), jnp.int32)
    for s in range(slots):
        episode = jnp.where(row == s, episode_s[mine * slots + s], episode)
        asked = jnp.where(row == s, flag_s[mine * slots + s], asked)
    picked = jnp.zeros((slots, WAYS), F32)
    for e in range(classes // WAYS):
        picked = jnp.where(episode == e, distance[:, e * WAYS : (e + 1) * WAYS], picked)
    logits = picked * (-1.0 / math.sqrt(width))
    shifted = logits - jnp.max(logits, axis=1, keepdims=True)
    result = shifted - jnp.log(jnp.sum(jnp.exp(shifted), axis=1, keepdims=True))
    log_ref[...] = jnp.where(asked == 1, result, 0.0)

    for copies in (reduce_early, reduce_late, copies_sq, copies_fin):
        for d in order:
            copies[d].wait_send()
    for group in range(2):
        for i in range(len(offsets)):
            gather_copy(group, i).wait_send()
        for i in range(len(offsets) + 1):
            relay_copy(group, i).wait_send()


def per_device(
    tokens,
    norm_gain,
    w_query,
    w_key,
    w_value,
    w_out,
    seq_starts,
    seq_lengths,
    episode_ids,
    class_ids,
    query_flags,
):
    rows, width = tokens.shape
    slots = seq_starts.shape[0]
    inner = w_query.shape[1]
    heads = inner // HEAD_DIM
    columns = inner + w_key.shape[1] + w_value.shape[1]
    mp, dp = lax.axis_size("mp"), lax.axis_size("dp")
    share = width // mp
    tiles = rows // TILE
    total = episode_ids.shape[0]
    classes = max(1, total // (2 * WAYS)) * WAYS
    chips = dp // 2
    late = (slots - EARLY) * PIECES
    fine, coarse = rope_tables(rows, 64)
    hbm = pl.BlockSpec(memory_space=pltpu.HBM)
    vmem = pl.BlockSpec(memory_space=pltpu.VMEM)
    dma = lambda *n: pltpu.SemaphoreType.DMA(n)
    ints = lambda n: pltpu.SMEM((n,), jnp.int32)
    return pl.pallas_call(
        whole_kernel,
        out_shape=(
            jax.ShapeDtypeStruct((slots, WAYS), F32),
            jax.ShapeDtypeStruct((classes, share), F32),
        ),
        in_specs=[hbm] * 13,
        out_specs=(vmem, vmem),
        scratch_shapes=[
            ints(slots),
            ints(slots),
            ints(total),
            ints(total),
            pltpu.VMEM((total,), jnp.int32),
            pltpu.VMEM((total,), jnp.int32),
            pltpu.VMEM((total,), jnp.int32),
            pltpu.VMEM((width,), BF16),
            pltpu.VMEM(fine.shape, F32),
            pltpu.VMEM(coarse.shape, F32),
            pltpu.VMEM((rows, width), BF16),
            pltpu.VMEM((width, columns), BF16),
            pltpu.VMEM((inner, width), BF16),
            pltpu.VMEM((rows, columns), F32),
            pltpu.VMEM((rows, 128), F32),
            pltpu.VMEM((ONES, rows), BF16),
            pltpu.VMEM((3, 256, heads * TILE), BF16),
            pltpu.VMEM((rows, 256), BF16),
            pltpu.VMEM((128 + ONES, rows), BF16),
            pltpu.VMEM((inner, rows), BF16),
            pltpu.VMEM((mp, EARLY * PIECES, share // PIECES), F32),
            pltpu.VMEM((mp - 1, EARLY * PIECES, share // PIECES), F32),
            pltpu.VMEM((dp, EARLY * PIECES, share // PIECES), F32),
            pltpu.VMEM((mp, late, share // PIECES), F32),
            pltpu.VMEM((mp - 1, mp, late, share // PIECES), F32),
            pltpu.VMEM((mp, late, share // PIECES), F32),
            pltpu.VMEM((dp, late, share // PIECES), F32),
            pltpu.VMEM((dp, 128), F32),
            pltpu.VMEM((mp - 1, dp, 128), F32),
            pltpu.VMEM((2 * slots, 128), F32),
            pltpu.VMEM((mp - 1, 2 * slots, 128), F32),
            dma(10),
            dma(STEPS + 1),
            dma(STEPS + 1),
            dma(STEPS + 1),
            dma(STEPS + 1),
            dma(1),
            dma(mp - 1),
            dma(mp - 1),
            dma(mp - 1),
            dma(mp - 1),
            dma(mp - 1),
            dma(mp - 1),
            dma(2, chips - 1),
            dma(2, chips - 1),
            dma(2, chips),
            dma(2, chips),
            dma(mp - 1),
            dma(mp - 1),
        ],
        compiler_params=pltpu.CompilerParams(
            collective_id=0, has_side_effects=True, vmem_limit_bytes=50 * 2**20
        ),
        name="whole",
    )(
        *(
            pltpu.with_memory_space_constraint(array, pltpu.HBM)
            for array in (
                seq_starts,
                seq_lengths,
                episode_ids,
                class_ids,
                query_flags,
                norm_gain,
                jnp.asarray(fine),
                jnp.asarray(coarse),
                tokens,
                w_query,
                w_key,
                w_value,
                w_out,
            )
        )
    )


def solution(mesh):
    placed = (
        P("dp", None),
        P(),
        P(None, "mp"),
        P(None, "mp"),
        P(None, "mp"),
        P("mp", None),
        P("dp"),
        P("dp"),
        P(),
        P(),
        P(),
    )
    return jax.shard_map(
        per_device,
        mesh=mesh,
        in_specs=placed,
        out_specs=(P("dp", None), P(None, "mp")),
        check_vma=False,
    )
```

```python
import functools
import math

import jax
import jax.numpy as jnp
import numpy as np
from jax import lax
from jax.experimental import pallas as pl
from jax.experimental.pallas import tpu as pltpu
from jax.sharding import PartitionSpec as P

HEAD_DIM = 128
WAYS = 32
ROPE_BASE = 500000.0
LONGEST = 640
STEPS = 8
AHEAD = 2
HELD = 6
TILE = 128
ONES = 16
EARLY = 4
PIECES = 2
BLOCK = 512
SHORTEST = 128
FAR = -(2.0**100)
F32 = jnp.float32
BF16 = jnp.bfloat16


def rope_tables(rows, block):
    half = HEAD_DIM // 2
    frequency = ROPE_BASE ** (-(np.arange(half, dtype=np.float64) * 2.0 / HEAD_DIM))
    frequency = np.concatenate([frequency, frequency])[None, :]
    sign = np.where(np.arange(HEAD_DIM) < half, -1.0, 1.0)[None, :]
    fine = np.arange(block, dtype=np.float64)[:, None] * frequency
    coarse = np.arange(0, rows, block, dtype=np.float64)[:, None] * frequency
    fine_table = np.stack([np.cos(fine), np.sin(fine)])
    coarse_table = np.stack(
        [np.cos(coarse), np.sin(coarse), sign * np.cos(coarse), sign * np.sin(coarse)]
    )
    return fine_table.astype(np.float32), coarse_table.astype(np.float32)


def dot(a, b):
    return jnp.dot(a, b, preferred_element_type=F32)


def dot_nt(a, b):
    return lax.dot_general(a, b, (((1,), (1,)), ((), ())), preferred_element_type=F32)


def split(a):
    high = a.astype(BF16)
    return high, (a - high.astype(F32)).astype(BF16)


def fold(a):
    span = a.shape[1] // PIECES
    return jnp.concatenate([a[:, p * span : (p + 1) * span] for p in range(PIECES)], axis=0)


def unfold(first, second):
    axis = first.ndim - 2
    size = first.shape[axis] // PIECES
    piece = lambda a, p: lax.slice_in_dim(a, p * size, (p + 1) * size, axis=axis)
    return jnp.concatenate(
        [
            jnp.concatenate([piece(first, p), piece(second, p)], axis=axis)
            for p in range(PIECES)
        ],
        axis=axis + 1,
    )


def whole_kernel(
    starts_h,
    lengths_h,
    episode_h,
    class_h,
    flag_h,
    gain_h,
    fine_h,
    coarse_h,
    x_h,
    wq_h,
    wk_h,
    wv_h,
    wo_h,
    log_ref,
    proto_ref,
    starts,
    lengths,
    episode_s,
    flag_s,
    episode_v,
    class_v,
    flag_v,
    gain,
    fine,
    coarse,
    x_v,
    w_v,
    wo_v,
    acc,
    squares,
    member,
    qt,
    ks,
    vt,
    ot,
    part,
    landed,
    everyone,
    square_part,
    square_landed,
    final_part,
    final_landed,
    small_sem,
    x_sem,
    wq_sem,
    wk_sem,
    wv_sem,
    wo_sem,
    rs_send,
    rs_recv,
    sq_send,
    sq_recv,
    ag_send,
    ag_recv,
    relay_send,
    relay_recv,
    fin_send,
    fin_recv,
):
    mp = lax.axis_size("mp")
    dp = lax.axis_size("dp")
    me = lax.axis_index("mp")
    mine = lax.axis_index("dp")
    rows, width = x_h.shape
    slots = starts.shape[0]
    heads = wq_h.shape[1] // HEAD_DIM
    depth = width // STEPS
    tiles = rows // TILE
    share = width // mp
    late = slots - EARLY
    cut = rows - late * SHORTEST
    late_from = EARLY * SHORTEST

    smalls = [
        pltpu.make_async_copy(source, target, small_sem.at[i])
        for i, (source, target) in enumerate(
            [
                (gain_h, gain),
                (starts_h, starts),
                (lengths_h, lengths),
                (fine_h, fine),
                (coarse_h, coarse),
                (episode_h, episode_s),
                (flag_h, flag_s),
                (episode_h, episode_v),
                (class_h, class_v),
                (flag_h, flag_v),
            ]
        )
    ]

    bounds = [(0, depth // 2), (depth // 2, depth // 2)]
    bounds += [(depth, depth)]
    bounds += [(c * depth, 2 * depth) for c in range(2, STEPS, 2)]

    def chunk_copies(c):
        at = pl.ds(*bounds[c])
        q, k = heads * HEAD_DIM, HEAD_DIM
        return [
            pltpu.make_async_copy(
                x_h.at[:, at], x_v.at[:, at], x_sem.at[c]
            ),
            pltpu.make_async_copy(wq_h.at[at, :], w_v.at[at, pl.ds(0, q)], wq_sem.at[c]),
            pltpu.make_async_copy(wk_h.at[at, :], w_v.at[at, pl.ds(q, k)], wk_sem.at[c]),
            pltpu.make_async_copy(wv_h.at[at, :], w_v.at[at, pl.ds(q + k, k)], wv_sem.at[c]),
        ]

    smalls[0].start()
    for copy in chunk_copies(0):
        copy.start()
    for copy in smalls[1:]:
        copy.start()
    for c in range(1, AHEAD):
        for copy in chunk_copies(c):
            copy.start()
    wo_copy = pltpu.make_async_copy(wo_h, wo_v, wo_sem.at[0])

    def lane_squares(x):
        wide = x.astype(F32)
        wide = wide * wide
        total = wide[:, 0:128]
        for i in range(1, x.shape[1] // 128):
            total += wide[:, i * 128 : (i + 1) * 128]
        return total

    def project_chunk(c):
        deep = pl.ds(*bounds[c])
        for first in range(0, rows, BLOCK):
            at = pl.ds(first, BLOCK)
            x = x_v[at, deep]
            value = dot(x * gain[deep].reshape(1, bounds[c][1]), w_v[deep, :])
            if c == 0:
                squares[at, :] = lane_squares(x)
                acc[at, :] = value
            else:
                squares[at, :] += lane_squares(x)
                acc[at, :] += value

    scale = math.log2(math.e) / math.sqrt(HEAD_DIM)

    def row_scale_of(at):
        return lax.rsqrt(jnp.sum(squares[at, :], axis=1, keepdims=True) * (1.0 / width) + 1e-05)

    def slot_bounds(shape, axis):
        index = lax.broadcasted_iota(jnp.int32, shape, axis)
        first = jnp.full(shape, rows, jnp.int32)
        last = jnp.zeros(shape, jnp.int32)
        for s in range(slots):
            first = jnp.where(index == s, starts[s], first)
            last = jnp.where(index == s, starts[s] + lengths[s], last)
        return first, last

    def prepare(i):
        first, last = slot_bounds((1, 128), 1)
        fine_cos, fine_sin = fine[0], fine[1]
        at = pl.ds(i * TILE, TILE)
        row_scale = row_scale_of(at)
        cosines, sines = [], []
        for b in range(i * TILE // 64, (i + 1) * TILE // 64):
            cos_a, sin_a = coarse[0, b : b + 1, :], coarse[1, b : b + 1, :]
            cos_s, sin_s = coarse[2, b : b + 1, :], coarse[3, b : b + 1, :]
            cosines.append(cos_a * fine_cos - sin_a * fine_sin)
            sines.append(sin_s * fine_cos + cos_s * fine_sin)
        cosine = jnp.concatenate(cosines, axis=0) * row_scale
        sine = jnp.concatenate(sines, axis=0) * row_scale
        for n in range(heads):
            v = acc[at, n * 128 : (n + 1) * 128]
            v = v * cosine + pltpu.roll(v, 64, 1) * sine
            qt[i % HELD, 0:128, n * TILE : (n + 1) * TILE] = v.T.astype(BF16)
            qt[i % HELD, 128 : 128 + ONES, n * TILE : (n + 1) * TILE] = member[:, at]
        v = acc[at, heads * 128 : (heads + 1) * 128] * scale
        v = v * cosine + pltpu.roll(v, 64, 1) * sine
        ks[at, 0:128] = v.astype(BF16)
        token = i * TILE + lax.broadcasted_iota(jnp.int32, (TILE, 128), 0)
        inside = (token >= first) & (token < last)
        ks[at, 128:256] = jnp.where(inside, 0.0, FAR).astype(BF16)
        v = acc[at, (heads + 1) * 128 : (heads + 2) * 128] * row_scale
        vt[0:128, at] = v.T.astype(BF16)
        vt[128 : 128 + ONES, at] = jnp.ones((ONES, TILE), BF16)

    def score(i):
        begin = max(0, i * TILE - LONGEST)
        return dot(ks[begin : (i + 1) * TILE, :], qt[i % HELD])

    def mix(i, s):
        key = lax.broadcasted_iota(jnp.int32, (TILE, heads * TILE), 0)
        query = lax.broadcasted_iota(jnp.int32, (TILE, heads * TILE), 1) % TILE
        begin = max(0, i * TILE - LONGEST)
        before = i * TILE - begin
        own = jnp.where(key <= query, s[before:], FAR)
        peak = jnp.max(own, axis=0, keepdims=True)
        if before:
            peak = jnp.maximum(peak, jnp.max(s[:before], axis=0, keepdims=True))
        e = jnp.exp2(own - peak).astype(BF16)
        if before:
            e = jnp.concatenate([jnp.exp2(s[:before] - peak).astype(BF16), e], axis=0)
        o = dot(vt[:, begin : (i + 1) * TILE], e)
        o = (o[0:128] / o[128:129]).astype(BF16)
        for n in range(heads):
            ot[n * 128 : (n + 1) * 128, i * TILE : (i + 1) * TILE] = o[:, n * TILE : (n + 1) * TILE]

    def attend(first, last):
        prepare(first)
        ready = score(first)
        for i in range(first, last):
            now = ready
            if i + 1 < last:
                prepare(i + 1)
                ready = score(i + 1)
            mix(i, now)

    spans = (slice(0, cut), slice(late_from, rows))
    picks = (slice(0, EARLY), slice(EARLY, slots))

    def head_part(group):
        span, pick = spans[group], picks[group]
        high, low = split(dot_nt(member[:, span], ot[:, span])[pick])
        stacked = jnp.concatenate([high, low], axis=0)
        for r in range(mp):
            both = dot(stacked, wo_v[:, r * share : (r + 1) * share])
            n = both.shape[0] // 2
            part[group, r] = fold(both[:n] + both[n:])

    def divided(value, first, size):
        row = lax.broadcasted_iota(jnp.int32, (value.shape[0], 1), 0)
        count = jnp.ones(row.shape, jnp.int32)
        for s in range(value.shape[0]):
            count = jnp.where(row == s, lengths[first + s % size], count)
        return value / count.astype(F32)

    order = sorted(range(1, mp), key=lambda d: -min(d, mp - d))

    def to_ranks(source, target, send, recv):
        return {
            d: pltpu.make_async_remote_copy(
                src_ref=source(d),
                dst_ref=target(d),
                send_sem=send(d),
                recv_sem=recv(d),
                device_id={"mp": (me + d) % mp},
            )
            for d in order
        }

    side = int(math.isqrt(dp // 2))
    x, y, core = mine // (2 * side), (mine // 2) % side, mine % 2
    partner = mine + 1 - 2 * core

    def at_offset(dx, dy):
        return (((x + dx + side) % side) * side + (y + dy + side) % side) * 2 + core

    reach = lambda o: min(o[0], side - o[0]) + min(o[1], side - o[1])
    offsets = [(dx, dy) for dx in range(side) for dy in range(side) if dx or dy]
    offsets = sorted(offsets, key=lambda o: -reach(o))

    def reduce_copies(group):
        return to_ranks(
            lambda d: part.at[group, (me + d) % mp],
            lambda d: landed.at[group, d - 1],
            lambda d: rs_send.at[group, d - 1],
            lambda d: rs_recv.at[group, d - 1],
        )

    def square_copies(group):
        return to_ranks(
            lambda d: square_part.at[group],
            lambda d: square_landed.at[group, d - 1],
            lambda d: sq_send.at[group, d - 1],
            lambda d: sq_recv.at[group, d - 1],
        )

    def token_part(group):
        own_features = pl.ds(pl.multiple_of(me * share, share), share)
        return fold(dot(member[:, spans[group]], x_v[spans[group], own_features])[picks[group]])

    lane = lax.broadcasted_iota(jnp.int32, (slots, 128), 1)
    slot = lax.broadcasted_iota(jnp.int32, (slots, 128), 0)

    def reduced(group, value, copies):
        value += part[group, me]
        for d in reversed(order):
            copies[d].wait_recv()
            value += landed[group, d - 1]
        value = divided(value, group * EARLY, EARLY)
        square = jnp.sum(value * value, axis=1, keepdims=True)
        square = jnp.sum(
            jnp.where(lane % EARLY == slot % EARLY, square, 0.0), axis=0, keepdims=True
        )
        square_part[group] = square
        sent = square_copies(group)
        for d in order:
            sent[d].start()
        return value, square, sent

    def embedded(group, value, square, sent):
        for d in reversed(order):
            sent[d].wait_recv()
            square += square_landed[group, d - 1]
        mean = jnp.sum(jnp.where(lane == slot % EARLY, square, 0.0), axis=1, keepdims=True)
        mean = mean * (1.0 / width)
        value = value * lax.rsqrt(mean + 1e-06)
        everyone[group, mine] = value
        gather(group)
        return value, mean

    def class_part(group):
        a = everyone[group]
        high = a.astype(BF16).astype(F32)
        both = unfold(high, a - high).astype(BF16).reshape(total, share)
        lanes = lax.broadcasted_iota(jnp.int32, (1, total), 1) % slots
        if group == 0:
            names = jnp.where(lanes < EARLY, named, pltpu.roll(named, EARLY, 1))
        else:
            names = jnp.where(lanes >= EARLY, named, pltpu.roll(named, total - EARLY, 1))
        kind = lax.broadcasted_iota(jnp.int32, (classes, total), 0)
        return dot(jnp.where(kind == names, 1.0, 0.0).astype(BF16), both)

    def gather_copy(group, i):
        return pltpu.make_async_remote_copy(
            src_ref=everyone.at[group, mine],
            dst_ref=everyone.at[group, mine],
            send_sem=ag_send.at[group, i],
            recv_sem=ag_recv.at[group, i],
            device_id={"dp": at_offset(*offsets[i])},
        )

    def relay_copy(group, i):
        source = mine if i == len(offsets) else at_offset(-offsets[i][0], -offsets[i][1])
        return pltpu.make_async_remote_copy(
            src_ref=everyone.at[group, source],
            dst_ref=everyone.at[group, source],
            send_sem=relay_send.at[group, i],
            recv_sem=relay_recv.at[group, i],
            device_id={"dp": partner},
        )

    def gather(group):
        for i in range(len(offsets)):
            gather_copy(group, i).start()
        relay_copy(group, len(offsets)).start()

    def relay(group):
        for i in reversed(range(len(offsets))):
            gather_copy(group, i).wait_recv()
            relay_copy(group, i).start()

    barrier = pltpu.get_barrier_semaphore()
    for d in range(1, mp):
        pl.semaphore_signal(barrier, inc=1, device_id={"mp": (me + d) % mp})
    for offset in offsets:
        pl.semaphore_signal(barrier, inc=1, device_id={"dp": at_offset(*offset)})
    pl.semaphore_signal(barrier, inc=1, device_id={"dp": partner})
    smalls[0].wait()
    for c in range(len(bounds)):
        for copy in chunk_copies(c):
            copy.wait()
        if c + AHEAD < len(bounds):
            for copy in chunk_copies(c + AHEAD):
                copy.start()
        elif c + AHEAD == len(bounds):
            wo_copy.start()
        project_chunk(c)
    for copy in smalls[1:]:
        copy.wait()
    token = lax.broadcasted_iota(jnp.int32, (ONES, rows), 1)
    first, last = slot_bounds((ONES, rows), 0)
    member[...] = jnp.where((token >= first) & (token < last), 1.0, 0.0).astype(BF16)
    qt[:, 128 + ONES :, :] = jnp.zeros((HELD, 128 - ONES, heads * TILE), BF16)
    attend(0, cut // TILE)
    wo_copy.wait()
    head_part(0)
    pl.semaphore_wait(barrier, mp - 1 + len(offsets) + 1)
    reduce_early = reduce_copies(0)
    for d in order:
        reduce_early[d].start()
    tokens_early = token_part(0)
    attend(cut // TILE, tiles)
    head_part(1)
    reduce_late = reduce_copies(1)
    for d in order:
        reduce_late[d].start()
    pooled_early, square_early, sent_early = reduced(0, tokens_early, reduce_early)
    tokens_late = token_part(1)
    total = dp * slots
    classes = proto_ref.shape[0]
    named = (episode_v[...] * WAYS + class_v[...]).reshape(1, total)
    named = jnp.where(flag_v[...].reshape(1, total) == 0, named, -1)
    own_early, mean_early = embedded(0, pooled_early, square_early, sent_early)
    pooled_late, square_late, sent_late = reduced(1, tokens_late, reduce_late)
    own_late, mean_late = embedded(1, pooled_late, square_late, sent_late)
    relay(0)
    own = unfold(own_early, own_late)
    own_mean = jnp.concatenate([mean_early[:EARLY], mean_late[:EARLY]], axis=0)
    own_weight = lax.rsqrt(own_mean + 1e-06)
    own_high, own_low = split(own)
    own = jnp.concatenate([own_high, own_low], axis=0)
    for i in range(len(offsets) + 1):
        relay_copy(0, i).wait_recv()
    sums = class_part(0)
    relay(1)
    for i in range(len(offsets) + 1):
        relay_copy(1, i).wait_recv()
    sums += class_part(1)
    sums_high, sums_low = split(sums)
    diagonal = lax.broadcasted_iota(jnp.int32, (classes, classes), 0) == lax.broadcasted_iota(
        jnp.int32, (classes, classes), 1
    )
    norms = jnp.sum(sums * sums, axis=1, keepdims=True)
    norms = jnp.sum(jnp.where(diagonal, norms, 0.0), axis=0, keepdims=True)
    cross = dot_nt(own, sums_high)
    cross = cross[:slots] + cross[slots:] + dot_nt(own, sums_low)[:slots]
    mixed = jnp.concatenate([cross, jnp.broadcast_to(norms, (slots, classes))], axis=0)
    final_part[...] = mixed
    copies_fin = to_ranks(
        lambda d: final_part,
        lambda d: final_landed.at[d - 1],
        lambda d: fin_send.at[d - 1],
        lambda d: fin_recv.at[d - 1],
    )
    for d in order:
        copies_fin[d].start()
    for d in reversed(order):
        copies_fin[d].wait_recv()
        mixed += final_landed[d - 1]
    class_mean = mixed[slots : slots + 1] * (1.0 / width)
    class_scale = lax.rsqrt(class_mean + 1e-06)
    column = jnp.sum(jnp.where(diagonal, class_scale, 0.0), axis=1, keepdims=True)
    proto_ref[...] = sums * column
    distance = (
        own_mean * own_weight * own_weight + class_mean * class_scale * class_scale
    ) * width - 2.0 * (mixed[:slots] * class_scale)
    row = lax.broadcasted_iota(jnp.int32, (slots, 1), 0)
    episode = jnp.zeros((slots, 1), jnp.int32)
    asked = jnp.zeros((slots, 1), jnp.int32)
    for s in range(slots):
        episode = jnp.where(row == s, episode_s[mine * slots + s], episode)
        asked = jnp.where(row == s, flag_s[mine * slots + s], asked)
    picked = jnp.zeros((slots, WAYS), F32)
    for e in range(classes // WAYS):
        picked = jnp.where(episode == e, distance[:, e * WAYS : (e + 1) * WAYS], picked)
    logits = picked * (-1.0 / math.sqrt(width))
    shifted = logits - jnp.max(logits, axis=1, keepdims=True)
    result = shifted - jnp.log(jnp.sum(jnp.exp(shifted), axis=1, keepdims=True))
    log_ref[...] = jnp.where(asked == 1, result, 0.0)

    for copies in (reduce_early, reduce_late, sent_early, sent_late, copies_fin):
        for d in order:
            copies[d].wait_send()
    for group in range(2):
        for i in range(len(offsets)):
            gather_copy(group, i).wait_send()
        for i in range(len(offsets) + 1):
            relay_copy(group, i).wait_send()


def per_device(
    tokens,
    norm_gain,
    w_query,
    w_key,
    w_value,
    w_out,
    seq_starts,
    seq_lengths,
    episode_ids,
    class_ids,
    query_flags,
):
    rows, width = tokens.shape
    slots = seq_starts.shape[0]
    inner = w_query.shape[1]
    heads = inner // HEAD_DIM
    columns = inner + w_key.shape[1] + w_value.shape[1]
    mp, dp = lax.axis_size("mp"), lax.axis_size("dp")
    share = width // mp
    tiles = rows // TILE
    total = episode_ids.shape[0]
    classes = max(1, total // (2 * WAYS)) * WAYS
    chips = dp // 2
    fine, coarse = rope_tables(rows, 64)
    hbm = pl.BlockSpec(memory_space=pltpu.HBM)
    vmem = pl.BlockSpec(memory_space=pltpu.VMEM)
    dma = lambda *n: pltpu.SemaphoreType.DMA(n)
    ints = lambda n: pltpu.SMEM((n,), jnp.int32)
    return pl.pallas_call(
        whole_kernel,
        out_shape=(
            jax.ShapeDtypeStruct((slots, WAYS), F32),
            jax.ShapeDtypeStruct((classes, share), F32),
        ),
        in_specs=[hbm] * 13,
        out_specs=(vmem, vmem),
        scratch_shapes=[
            ints(slots),
            ints(slots),
            ints(total),
            ints(total),
            pltpu.VMEM((total,), jnp.int32),
            pltpu.VMEM((total,), jnp.int32),
            pltpu.VMEM((total,), jnp.int32),
            pltpu.VMEM((width,), BF16),
            pltpu.VMEM(fine.shape, F32),
            pltpu.VMEM(coarse.shape, F32),
            pltpu.VMEM((rows, width), BF16),
            pltpu.VMEM((width, columns), BF16),
            pltpu.VMEM((inner, width), BF16),
            pltpu.VMEM((rows, columns), F32),
            pltpu.VMEM((rows, 128), F32),
            pltpu.VMEM((ONES, rows), BF16),
            pltpu.VMEM((HELD, 256, heads * TILE), BF16),
            pltpu.VMEM((rows, 256), BF16),
            pltpu.VMEM((128 + ONES, rows), BF16),
            pltpu.VMEM((inner, rows), BF16),
            pltpu.VMEM((2, mp, slots, share // PIECES), F32),
            pltpu.VMEM((2, mp - 1, slots, share // PIECES), F32),
            pltpu.VMEM((2, dp, slots, share // PIECES), F32),
            pltpu.VMEM((2, 1, 128), F32),
            pltpu.VMEM((2, mp - 1, 1, 128), F32),
            pltpu.VMEM((2 * slots, 128), F32),
            pltpu.VMEM((mp - 1, 2 * slots, 128), F32),
            dma(10),
            dma(STEPS + 1),
            dma(STEPS + 1),
            dma(STEPS + 1),
            dma(STEPS + 1),
            dma(1),
            dma(2, mp - 1),
            dma(2, mp - 1),
            dma(2, mp - 1),
            dma(2, mp - 1),
            dma(2, chips - 1),
            dma(2, chips - 1),
            dma(2, chips),
            dma(2, chips),
            dma(mp - 1),
            dma(mp - 1),
        ],
        compiler_params=pltpu.CompilerParams(
            collective_id=0, has_side_effects=True, vmem_limit_bytes=50 * 2**20
        ),
        name="whole",
    )(
        *(
            pltpu.with_memory_space_constraint(array, pltpu.HBM)
            for array in (
                seq_starts,
                seq_lengths,
                episode_ids,
                class_ids,
                query_flags,
                norm_gain,
                jnp.asarray(fine),
                jnp.asarray(coarse),
                tokens,
                w_query,
                w_key,
                w_value,
                w_out,
            )
        )
    )


def solution(mesh):
    placed = (
        P("dp", None),
        P(),
        P(None, "mp"),
        P(None, "mp"),
        P(None, "mp"),
        P("mp", None),
        P("dp"),
        P("dp"),
        P(),
        P(),
        P(),
    )
    return jax.shard_map(
        per_device,
        mesh=mesh,
        in_specs=placed,
        out_specs=(P("dp", None), P(None, "mp")),
        check_vma=False,
    )
```

```python
import functools
import math

import jax
import jax.numpy as jnp
import numpy as np
from jax import lax
from jax.experimental import pallas as pl
from jax.experimental.pallas import tpu as pltpu
from jax.sharding import PartitionSpec as P

HEAD_DIM = 128
WAYS = 32
ROPE_BASE = 500000.0
LONGEST = 640
STEPS = 8
AHEAD = 3
HELD = 12
TILE = 128
ONES = 16
EARLY = 4
PIECES = 2
BLOCK = 512
SHORTEST = 128
FAR = -(2.0**100)
F32 = jnp.float32
BF16 = jnp.bfloat16


def rope_tables(rows, block):
    half = HEAD_DIM // 2
    frequency = ROPE_BASE ** (-(np.arange(half, dtype=np.float64) * 2.0 / HEAD_DIM))
    frequency = np.concatenate([frequency, frequency])[None, :]
    sign = np.where(np.arange(HEAD_DIM) < half, -1.0, 1.0)[None, :]
    fine = np.arange(block, dtype=np.float64)[:, None] * frequency
    coarse = np.arange(0, rows, block, dtype=np.float64)[:, None] * frequency
    fine_table = np.stack([np.cos(fine), np.sin(fine)])
    coarse_table = np.stack(
        [np.cos(coarse), np.sin(coarse), sign * np.cos(coarse), sign * np.sin(coarse)]
    )
    return fine_table.astype(np.float32), coarse_table.astype(np.float32)


def dot(a, b):
    return jnp.dot(a, b, preferred_element_type=F32)


def dot_nt(a, b):
    return lax.dot_general(a, b, (((1,), (1,)), ((), ())), preferred_element_type=F32)


def split(a):
    high = a.astype(BF16)
    return high, (a - high.astype(F32)).astype(BF16)


def fold(a):
    span = a.shape[1] // PIECES
    return jnp.concatenate([a[:, p * span : (p + 1) * span] for p in range(PIECES)], axis=0)


def unfold(a, before, after):
    axis = a.ndim - 2
    size = a.shape[axis] // PIECES
    pad = lambda n: [jnp.zeros(a.shape[:axis] + (n, a.shape[-1]), a.dtype)] if n else []
    pieces = [
        jnp.concatenate(
            pad(before)
            + [lax.slice_in_dim(a, p * size, (p + 1) * size, axis=axis)]
            + pad(after),
            axis=axis,
        )
        for p in range(PIECES)
    ]
    return jnp.concatenate(pieces, axis=axis + 1)


def whole_kernel(
    starts_h,
    lengths_h,
    episode_h,
    class_h,
    flag_h,
    gain_h,
    fine_h,
    coarse_h,
    x_h,
    wq_h,
    wk_h,
    wv_h,
    wo_h,
    log_ref,
    sums_ref,
    column_ref,
    starts,
    lengths,
    episode_s,
    flag_s,
    episode_v,
    class_v,
    flag_v,
    gain,
    fine,
    coarse,
    x_v,
    w_v,
    wo_v,
    acc,
    squares,
    member,
    qt,
    ks,
    vt,
    ot,
    part,
    landed,
    everyone,
    late_part,
    late_landed,
    late_total,
    late_everyone,
    square_part,
    square_landed,
    final_part,
    final_landed,
    small_sem,
    x_sem,
    wq_sem,
    wk_sem,
    wv_sem,
    wo_sem,
    rs_send,
    rs_recv,
    ar_send,
    ar_recv,
    sq_send,
    sq_recv,
    ag_send,
    ag_recv,
    relay_send,
    relay_recv,
    fin_send,
    fin_recv,
):
    mp = lax.axis_size("mp")
    dp = lax.axis_size("dp")
    me = lax.axis_index("mp")
    mine = lax.axis_index("dp")
    rows, width = x_h.shape
    slots = starts.shape[0]
    heads = wq_h.shape[1] // HEAD_DIM
    depth = width // STEPS
    tiles = rows // TILE
    share = width // mp
    late = slots - EARLY
    late_rows = late
    cut = rows - late * SHORTEST
    late_from = EARLY * SHORTEST

    smalls = [
        pltpu.make_async_copy(source, target, small_sem.at[i])
        for i, (source, target) in enumerate(
            [
                (gain_h, gain),
                (starts_h, starts),
                (lengths_h, lengths),
                (fine_h, fine),
                (coarse_h, coarse),
                (episode_h, episode_s),
                (flag_h, flag_s),
                (episode_h, episode_v),
                (class_h, class_v),
                (flag_h, flag_v),
            ]
        )
    ]

    bounds = [(0, depth // 2), (depth // 2, depth // 2)]
    bounds += [(depth, depth)]
    bounds += [(c * depth, 2 * depth) for c in range(2, STEPS, 2)]

    def chunk_copies(c):
        at = pl.ds(*bounds[c])
        q, k = heads * HEAD_DIM, HEAD_DIM
        return [
            pltpu.make_async_copy(
                x_h.at[:, at], x_v.at[:, at], x_sem.at[c]
            ),
            pltpu.make_async_copy(wq_h.at[at, :], w_v.at[at, pl.ds(0, q)], wq_sem.at[c]),
            pltpu.make_async_copy(wk_h.at[at, :], w_v.at[at, pl.ds(q, k)], wk_sem.at[c]),
            pltpu.make_async_copy(wv_h.at[at, :], w_v.at[at, pl.ds(q + k, k)], wv_sem.at[c]),
        ]

    smalls[0].start()
    for copy in chunk_copies(0):
        copy.start()
    for copy in smalls[1:]:
        copy.start()
    for c in range(1, AHEAD):
        for copy in chunk_copies(c):
            copy.start()
    wo_copy = pltpu.make_async_copy(wo_h, wo_v, wo_sem.at[0])

    def lane_squares(x):
        wide = x.astype(F32)
        wide = wide * wide
        total = wide[:, 0:128]
        for i in range(1, x.shape[1] // 128):
            total += wide[:, i * 128 : (i + 1) * 128]
        return total

    def project_chunk(c):
        deep = pl.ds(*bounds[c])
        for first in range(0, rows, BLOCK):
            at = pl.ds(first, BLOCK)
            x = x_v[at, deep]
            value = dot(x * gain[deep].reshape(1, bounds[c][1]), w_v[deep, :])
            if c == 0:
                squares[at, :] = lane_squares(x)
                acc[at, :] = value
            else:
                squares[at, :] += lane_squares(x)
                acc[at, :] += value

    scale = math.log2(math.e) / math.sqrt(HEAD_DIM)

    def row_scale_of(at):
        return lax.rsqrt(jnp.sum(squares[at, :], axis=1, keepdims=True) * (1.0 / width) + 1e-05)

    def slot_bounds(shape, axis):
        index = lax.broadcasted_iota(jnp.int32, shape, axis)
        first = jnp.full(shape, rows, jnp.int32)
        last = jnp.zeros(shape, jnp.int32)
        for s in range(slots):
            first = jnp.where(index == s, starts[s], first)
            last = jnp.where(index == s, starts[s] + lengths[s], last)
        return first, last

    def prepare(i):
        first, last = slot_bounds((1, 128), 1)
        fine_cos, fine_sin = fine[0], fine[1]
        at = pl.ds(i * TILE, TILE)
        row_scale = row_scale_of(at)
        cosines, sines = [], []
        for b in range(i * TILE // 64, (i + 1) * TILE // 64):
            cos_a, sin_a = coarse[0, b : b + 1, :], coarse[1, b : b + 1, :]
            cos_s, sin_s = coarse[2, b : b + 1, :], coarse[3, b : b + 1, :]
            cosines.append(cos_a * fine_cos - sin_a * fine_sin)
            sines.append(sin_s * fine_cos + cos_s * fine_sin)
        cosine = jnp.concatenate(cosines, axis=0) * row_scale
        sine = jnp.concatenate(sines, axis=0) * row_scale
        for n in range(heads):
            v = acc[at, n * 128 : (n + 1) * 128]
            v = v * cosine + pltpu.roll(v, 64, 1) * sine
            qt[i % HELD, 0:128, n * TILE : (n + 1) * TILE] = v.T.astype(BF16)
            qt[i % HELD, 128 : 128 + ONES, n * TILE : (n + 1) * TILE] = member[:, at]
        v = acc[at, heads * 128 : (heads + 1) * 128] * scale
        v = v * cosine + pltpu.roll(v, 64, 1) * sine
        ks[at, 0:128] = v.astype(BF16)
        token = i * TILE + lax.broadcasted_iota(jnp.int32, (TILE, 128), 0)
        inside = (token >= first) & (token < last)
        ks[at, 128:256] = jnp.where(inside, 0.0, FAR).astype(BF16)
        v = acc[at, (heads + 1) * 128 : (heads + 2) * 128] * row_scale
        vt[0:128, at] = v.T.astype(BF16)
        vt[128 : 128 + ONES, at] = jnp.ones((ONES, TILE), BF16)

    def score(i):
        begin = max(0, i * TILE - LONGEST)
        return dot(ks[begin : (i + 1) * TILE, :], qt[i % HELD])

    def mix(i, s):
        key = lax.broadcasted_iota(jnp.int32, (TILE, heads * TILE), 0)
        query = lax.broadcasted_iota(jnp.int32, (TILE, heads * TILE), 1) % TILE
        begin = max(0, i * TILE - LONGEST)
        before = i * TILE - begin
        own = jnp.where(key <= query, s[before:], FAR)
        peak = jnp.max(own, axis=0, keepdims=True)
        if before:
            peak = jnp.maximum(peak, jnp.max(s[:before], axis=0, keepdims=True))
        e = jnp.exp2(own - peak).astype(BF16)
        if before:
            e = jnp.concatenate([jnp.exp2(s[:before] - peak).astype(BF16), e], axis=0)
        o = dot(vt[:, begin : (i + 1) * TILE], e)
        o = (o[0:128] / o[128:129]).astype(BF16)
        for n in range(heads):
            ot[n * 128 : (n + 1) * 128, i * TILE : (i + 1) * TILE] = o[:, n * TILE : (n + 1) * TILE]

    def attend(first, last):
        prepare(first)
        ready = score(first)
        for i in range(first, last):
            now = ready
            if i + 1 < last:
                prepare(i + 1)
                ready = score(i + 1)
            mix(i, now)

    def head_part(span, pick, target):
        high, low = split(dot_nt(member[:, span], ot[:, span])[pick])
        stacked = jnp.concatenate([high, low], axis=0)
        for r in range(mp):
            both = dot(stacked, wo_v[:, r * share : (r + 1) * share])
            n = both.shape[0] // 2
            target[r] = fold(both[:n] + both[n:])

    def divided(value, first, size):
        row = lax.broadcasted_iota(jnp.int32, (value.shape[0], 1), 0)
        count = jnp.ones(row.shape, jnp.int32)
        for s in range(value.shape[0]):
            count = jnp.where(row == s, lengths[first + s % size], count)
        return value / count.astype(F32)

    order = sorted(range(1, mp), key=lambda d: -min(d, mp - d))

    def to_ranks(source, target, send, recv):
        return {
            d: pltpu.make_async_remote_copy(
                src_ref=source(d),
                dst_ref=target.at[d - 1],
                send_sem=send.at[d - 1],
                recv_sem=recv.at[d - 1],
                device_id={"mp": (me + d) % mp},
            )
            for d in order
        }

    side = int(math.isqrt(dp // 2))
    x, y, core = mine // (2 * side), (mine // 2) % side, mine % 2
    partner = mine + 1 - 2 * core

    def at_offset(dx, dy):
        return (((x + dx + side) % side) * side + (y + dy + side) % side) * 2 + core

    reach = lambda o: min(o[0], side - o[0]) + min(o[1], side - o[1])
    offsets = [(dx, dy) for dx in range(side) for dy in range(side) if dx or dy]
    offsets = sorted(offsets, key=lambda o: -reach(o))

    gathered = (everyone, late_everyone)

    def gather_copy(group, i):
        return pltpu.make_async_remote_copy(
            src_ref=gathered[group].at[mine],
            dst_ref=gathered[group].at[mine],
            send_sem=ag_send.at[group, i],
            recv_sem=ag_recv.at[group, i],
            device_id={"dp": at_offset(*offsets[i])},
        )

    def relay_copy(group, i):
        source = mine if i == len(offsets) else at_offset(-offsets[i][0], -offsets[i][1])
        return pltpu.make_async_remote_copy(
            src_ref=gathered[group].at[source],
            dst_ref=gathered[group].at[source],
            send_sem=relay_send.at[group, i],
            recv_sem=relay_recv.at[group, i],
            device_id={"dp": partner},
        )

    def gather(group):
        for i in range(len(offsets)):
            gather_copy(group, i).start()
        relay_copy(group, len(offsets)).start()

    def relay(group):
        for i in reversed(range(len(offsets))):
            gather_copy(group, i).wait_recv()
            relay_copy(group, i).start()

    barrier = pltpu.get_barrier_semaphore()
    for d in range(1, mp):
        pl.semaphore_signal(barrier, inc=1, device_id={"mp": (me + d) % mp})
    for offset in offsets:
        pl.semaphore_signal(barrier, inc=1, device_id={"dp": at_offset(*offset)})
    pl.semaphore_signal(barrier, inc=1, device_id={"dp": partner})
    smalls[0].wait()
    for c in range(len(bounds)):
        for copy in chunk_copies(c):
            copy.wait()
        if c + AHEAD < len(bounds):
            for copy in chunk_copies(c + AHEAD):
                copy.start()
        elif c + AHEAD == len(bounds):
            wo_copy.start()
        project_chunk(c)
    for copy in smalls[1:]:
        copy.wait()
    token = lax.broadcasted_iota(jnp.int32, (ONES, rows), 1)
    first, last = slot_bounds((ONES, rows), 0)
    member[...] = jnp.where((token >= first) & (token < last), 1.0, 0.0).astype(BF16)
    qt[:, 128 + ONES :, :] = jnp.zeros((HELD, 128 - ONES, heads * TILE), BF16)
    attend(0, cut // TILE)
    wo_copy.wait()
    head_part(slice(0, cut), slice(0, EARLY), part)
    pl.semaphore_wait(barrier, mp - 1 + len(offsets) + 1)
    reduce_early = to_ranks(lambda d: part.at[(me + d) % mp], landed, rs_send, rs_recv)
    for d in order:
        reduce_early[d].start()

    own_features = pl.ds(pl.multiple_of(me * share, share), share)
    pooled = fold(dot(member[:, :cut], x_v[:cut, own_features])[:EARLY])
    attend(cut // TILE, tiles)
    head_part(slice(late_from, rows), slice(EARLY, slots), late_part)
    reduce_late = to_ranks(lambda d: late_part, late_landed, ar_send, ar_recv)
    for d in order:
        reduce_late[d].start()

    pooled += part[me]
    for d in reversed(order):
        reduce_early[d].wait_recv()
        pooled += landed[d - 1]
    pooled = divided(pooled, 0, EARLY)
    everyone[mine] = pooled
    gather(0)
    late_tokens = dot(member[:, late_from:], x_v[late_from:, :])[EARLY:slots]
    for r in range(mp):
        late_total[r] = fold(late_tokens[:, r * share : (r + 1) * share]) + late_part[r]
    total = dp * slots
    classes = sums_ref.shape[0]
    named = episode_v[...] * WAYS + class_v[...]
    named = jnp.where(flag_v[...] == 0, named, -1).reshape(1, total)
    kind = lax.broadcasted_iota(jnp.int32, (classes, total), 0)
    select = jnp.where(kind == named, 1.0, 0.0).astype(BF16)
    for d in reversed(order):
        reduce_late[d].wait_recv()
    late_square = jnp.zeros((late_rows * PIECES, 1), F32)
    for r in range(mp):
        value = late_total[r]
        for d in order:
            value += late_landed[d - 1, r]
        value = divided(value, EARLY, late_rows)
        late_total[r] = value
        late_square += jnp.sum(value * value, axis=1, keepdims=True)
    lane = lax.broadcasted_iota(jnp.int32, (slots, 128), 1)
    slot = lax.broadcasted_iota(jnp.int32, (slots, 128), 0)
    late_square = jnp.sum(
        jnp.where(lane % late_rows == slot % late_rows, late_square, 0.0), axis=0, keepdims=True
    )
    late_mean = jnp.sum(
        jnp.where(lane == slot % late_rows, late_square, 0.0), axis=1, keepdims=True
    ) * (1.0 / width)
    late_own = late_total[me] * lax.rsqrt(late_mean + 1e-06)
    late_everyone[mine] = late_own
    gather(1)

    relay(0)
    for i in range(len(offsets) + 1):
        relay_copy(0, i).wait_recv()
    early = unfold(everyone[...], 0, late_rows)
    square = jnp.sum(early * early, axis=2, keepdims=True)
    wide_lane = lax.broadcasted_iota(jnp.int32, (dp, slots, 128), 2)
    wide_slot = lax.broadcasted_iota(jnp.int32, (dp, slots, 128), 1)
    square = jnp.sum(jnp.where(wide_lane == wide_slot, square, 0.0), axis=1)
    square_part[...] = square
    copies_sq = to_ranks(lambda d: square_part, square_landed, sq_send, sq_recv)
    for d in order:
        copies_sq[d].start()
    relay(1)
    for d in reversed(order):
        copies_sq[d].wait_recv()
        square += square_landed[d - 1]
    square_part_total = square.reshape(dp, 1, 128)
    mean = jnp.sum(
        jnp.where(wide_lane == wide_slot, square_part_total, 0.0), axis=2, keepdims=True
    ) * (1.0 / width)
    high, low = split((early * lax.rsqrt(mean + 1e-06)).reshape(total, share))
    sums = dot(select, high) + dot(select, low)
    own_row = lax.broadcasted_iota(jnp.int32, (dp, 128), 0) == mine
    own_square = jnp.sum(jnp.where(own_row, square, 0.0), axis=0, keepdims=True)
    own_square = jnp.where(slot >= EARLY, late_square, own_square)
    own_mean = jnp.sum(jnp.where(lane == slot, own_square, 0.0), axis=1, keepdims=True) * (
        1.0 / width
    )
    own_weight = lax.rsqrt(own_mean + 1e-06)
    own = unfold(pooled, 0, late_rows) * own_weight + unfold(late_own, EARLY, 0)
    own_high, own_low = split(own)
    own = jnp.concatenate([own_high, own_low], axis=0)
    for i in range(len(offsets) + 1):
        relay_copy(1, i).wait_recv()
    high, low = split(unfold(late_everyone[...], EARLY, 0).reshape(total, share))
    sums += dot(select, high) + dot(select, low)
    sums_high, sums_low = split(sums)
    diagonal = lax.broadcasted_iota(jnp.int32, (classes, classes), 0) == lax.broadcasted_iota(
        jnp.int32, (classes, classes), 1
    )
    norms = jnp.sum(sums * sums, axis=1, keepdims=True)
    norms = jnp.sum(jnp.where(diagonal, norms, 0.0), axis=0, keepdims=True)
    cross = dot_nt(own, sums_high)
    cross = cross[:slots] + cross[slots:] + dot_nt(own, sums_low)[:slots]
    mixed = jnp.concatenate([cross, jnp.broadcast_to(norms, (slots, classes))], axis=0)
    final_part[...] = mixed
    copies_fin = to_ranks(lambda d: final_part, final_landed, fin_send, fin_recv)
    for d in order:
        copies_fin[d].start()
    sums_ref[...] = sums
    for d in reversed(order):
        copies_fin[d].wait_recv()
        mixed += final_landed[d - 1]
    class_mean = mixed[slots : slots + 1] * (1.0 / width)
    class_scale = lax.rsqrt(class_mean + 1e-06)
    column = jnp.sum(jnp.where(diagonal, class_scale, 0.0), axis=1, keepdims=True)
    column_ref[...] = jnp.broadcast_to(column, column_ref.shape)
    distance = (
        own_mean * own_weight * own_weight + class_mean * class_scale * class_scale
    ) * width - 2.0 * (mixed[:slots] * class_scale)
    row = lax.broadcasted_iota(jnp.int32, (slots, 1), 0)
    episode = jnp.zeros((slots, 1), jnp.int32)
    asked = jnp.zeros((slots, 1), jnp.int32)
    for s in range(slots):
        episode = jnp.where(row == s, episode_s[mine * slots + s], episode)
        asked = jnp.where(row == s, flag_s[mine * slots + s], asked)
    picked = jnp.zeros((slots, WAYS), F32)
    for e in range(classes // WAYS):
        picked = jnp.where(episode == e, distance[:, e * WAYS : (e + 1) * WAYS], picked)
    logits = picked * (-1.0 / math.sqrt(width))
    shifted = logits - jnp.max(logits, axis=1, keepdims=True)
    result = shifted - jnp.log(jnp.sum(jnp.exp(shifted), axis=1, keepdims=True))
    log_ref[...] = jnp.where(asked == 1, result, 0.0)

    for copies in (reduce_early, reduce_late, copies_sq, copies_fin):
        for d in order:
            copies[d].wait_send()
    for group in range(2):
        for i in range(len(offsets)):
            gather_copy(group, i).wait_send()
        for i in range(len(offsets) + 1):
            relay_copy(group, i).wait_send()


def deliver_kernel(log_in, sums, column, log_ref, proto_ref):
    log_ref[...] = log_in[...]
    scale = column[...]
    for c in range(0, sums.shape[1], scale.shape[1]):
        at = pl.ds(c, scale.shape[1])
        proto_ref[:, at] = sums[:, at] * scale


def per_device(
    tokens,
    norm_gain,
    w_query,
    w_key,
    w_value,
    w_out,
    seq_starts,
    seq_lengths,
    episode_ids,
    class_ids,
    query_flags,
):
    rows, width = tokens.shape
    slots = seq_starts.shape[0]
    inner = w_query.shape[1]
    heads = inner // HEAD_DIM
    columns = inner + w_key.shape[1] + w_value.shape[1]
    mp, dp = lax.axis_size("mp"), lax.axis_size("dp")
    share = width // mp
    tiles = rows // TILE
    total = episode_ids.shape[0]
    classes = max(1, total // (2 * WAYS)) * WAYS
    chips = dp // 2
    late = (slots - EARLY) * PIECES
    fine, coarse = rope_tables(rows, 64)
    hbm = pl.BlockSpec(memory_space=pltpu.HBM)
    vmem = pl.BlockSpec(memory_space=pltpu.VMEM)
    dma = lambda *n: pltpu.SemaphoreType.DMA(n)
    ints = lambda n: pltpu.SMEM((n,), jnp.int32)
    log_probs, sums, column = pl.pallas_call(
        whole_kernel,
        out_shape=(
            jax.ShapeDtypeStruct((slots, WAYS), F32),
            jax.ShapeDtypeStruct((classes, share), F32),
            jax.ShapeDtypeStruct((classes, 128), F32),
        ),
        in_specs=[hbm] * 13,
        out_specs=(vmem, vmem, vmem),
        scratch_shapes=[
            ints(slots),
            ints(slots),
            ints(total),
            ints(total),
            pltpu.VMEM((total,), jnp.int32),
            pltpu.VMEM((total,), jnp.int32),
            pltpu.VMEM((total,), jnp.int32),
            pltpu.VMEM((width,), BF16),
            pltpu.VMEM(fine.shape, F32),
            pltpu.VMEM(coarse.shape, F32),
            pltpu.VMEM((rows, width), BF16),
            pltpu.VMEM((width, columns), BF16),
            pltpu.VMEM((inner, width), BF16),
            pltpu.VMEM((rows, columns), F32),
            pltpu.VMEM((rows, 128), F32),
            pltpu.VMEM((ONES, rows), BF16),
            pltpu.VMEM((HELD, 256, heads * TILE), BF16),
            pltpu.VMEM((rows, 256), BF16),
            pltpu.VMEM((128 + ONES, rows), BF16),
            pltpu.VMEM((inner, rows), BF16),
            pltpu.VMEM((mp, EARLY * PIECES, share // PIECES), F32),
            pltpu.VMEM((mp - 1, EARLY * PIECES, share // PIECES), F32),
            pltpu.VMEM((dp, EARLY * PIECES, share // PIECES), F32),
            pltpu.VMEM((mp, late, share // PIECES), F32),
            pltpu.VMEM((mp - 1, mp, late, share // PIECES), F32),
            pltpu.VMEM((mp, late, share // PIECES), F32),
            pltpu.VMEM((dp, late, share // PIECES), F32),
            pltpu.VMEM((dp, 128), F32),
            pltpu.VMEM((mp - 1, dp, 128), F32),
            pltpu.VMEM((2 * slots, 128), F32),
            pltpu.VMEM((mp - 1, 2 * slots, 128), F32),
            dma(10),
            dma(STEPS + 1),
            dma(STEPS + 1),
            dma(STEPS + 1),
            dma(STEPS + 1),
            dma(1),
            dma(mp - 1),
            dma(mp - 1),
            dma(mp - 1),
            dma(mp - 1),
            dma(mp - 1),
            dma(mp - 1),
            dma(2, chips - 1),
            dma(2, chips - 1),
            dma(2, chips),
            dma(2, chips),
            dma(mp - 1),
            dma(mp - 1),
        ],
        compiler_params=pltpu.CompilerParams(
            collective_id=0, has_side_effects=True, vmem_limit_bytes=50 * 2**20
        ),
        name="whole",
    )(
        *(
            pltpu.with_memory_space_constraint(array, pltpu.HBM)
            for array in (
                seq_starts,
                seq_lengths,
                episode_ids,
                class_ids,
                query_flags,
                norm_gain,
                jnp.asarray(fine),
                jnp.asarray(coarse),
                tokens,
                w_query,
                w_key,
                w_value,
                w_out,
            )
        )
    )
    return pl.pallas_call(
        deliver_kernel,
        out_shape=(
            jax.ShapeDtypeStruct((slots, WAYS), F32),
            jax.ShapeDtypeStruct((classes, share), F32),
        ),
        in_specs=[vmem] * 3,
        out_specs=(vmem, vmem),
        compiler_params=pltpu.CompilerParams(vmem_limit_bytes=8 * 2**20),
        name="deliver",
    )(log_probs, sums, column)


def solution(mesh):
    placed = (
        P("dp", None),
        P(),
        P(None, "mp"),
        P(None, "mp"),
        P(None, "mp"),
        P("mp", None),
        P("dp"),
        P("dp"),
        P(),
        P(),
        P(),
    )
    return jax.shard_map(
        per_device,
        mesh=mesh,
        in_specs=placed,
        out_specs=(P("dp", None), P(None, "mp")),
        check_vma=False,
    )
```

```python
import functools
import math

import jax
import jax.numpy as jnp
import numpy as np
from jax import lax
from jax.experimental import pallas as pl
from jax.experimental.pallas import tpu as pltpu
from jax.sharding import PartitionSpec as P

HEAD_DIM = 128
WAYS = 32
ROPE_BASE = 500000.0
LONGEST = 640
STEPS = 8
AHEAD = 3
HELD = 12
TILE = 128
ONES = 16
EARLY = 4
PIECES = 2
BLOCK = 512
SHORTEST = 128
FAR = -(2.0**100)
F32 = jnp.float32
BF16 = jnp.bfloat16


def rope_tables(rows, block):
    half = HEAD_DIM // 2
    frequency = ROPE_BASE ** (-(np.arange(half, dtype=np.float64) * 2.0 / HEAD_DIM))
    frequency = np.concatenate([frequency, frequency])[None, :]
    sign = np.where(np.arange(HEAD_DIM) < half, -1.0, 1.0)[None, :]
    fine = np.arange(block, dtype=np.float64)[:, None] * frequency
    coarse = np.arange(0, rows, block, dtype=np.float64)[:, None] * frequency
    fine_table = np.stack([np.cos(fine), np.sin(fine)])
    coarse_table = np.stack(
        [np.cos(coarse), np.sin(coarse), sign * np.cos(coarse), sign * np.sin(coarse)]
    )
    return fine_table.astype(np.float32), coarse_table.astype(np.float32)


def dot(a, b):
    return jnp.dot(a, b, preferred_element_type=F32)


def dot_nt(a, b):
    return lax.dot_general(a, b, (((1,), (1,)), ((), ())), preferred_element_type=F32)


def split(a):
    high = a.astype(BF16)
    return high, (a - high.astype(F32)).astype(BF16)


def fold(a):
    span = a.shape[1] // PIECES
    return jnp.concatenate([a[:, p * span : (p + 1) * span] for p in range(PIECES)], axis=0)


def unfold(a, before, after):
    axis = a.ndim - 2
    size = a.shape[axis] // PIECES
    pad = lambda n: [jnp.zeros(a.shape[:axis] + (n, a.shape[-1]), a.dtype)] if n else []
    pieces = [
        jnp.concatenate(
            pad(before)
            + [lax.slice_in_dim(a, p * size, (p + 1) * size, axis=axis)]
            + pad(after),
            axis=axis,
        )
        for p in range(PIECES)
    ]
    return jnp.concatenate(pieces, axis=axis + 1)


def whole_kernel(
    starts_h,
    lengths_h,
    episode_h,
    class_h,
    flag_h,
    gain_h,
    fine_h,
    coarse_h,
    x_h,
    wq_h,
    wk_h,
    wv_h,
    wo_h,
    log_ref,
    sums_ref,
    column_ref,
    starts,
    lengths,
    episode_s,
    flag_s,
    episode_v,
    class_v,
    flag_v,
    gain,
    fine,
    coarse,
    x_v,
    w_v,
    wo_v,
    acc,
    squares,
    member,
    qt,
    ks,
    vt,
    ot,
    part,
    landed,
    everyone,
    late_part,
    late_landed,
    late_total,
    late_everyone,
    square_part,
    square_landed,
    final_part,
    final_landed,
    small_sem,
    x_sem,
    wq_sem,
    wk_sem,
    wv_sem,
    wo_sem,
    rs_send,
    rs_recv,
    ar_send,
    ar_recv,
    sq_send,
    sq_recv,
    ag_send,
    ag_recv,
    relay_send,
    relay_recv,
    fin_send,
    fin_recv,
):
    mp = lax.axis_size("mp")
    dp = lax.axis_size("dp")
    me = lax.axis_index("mp")
    mine = lax.axis_index("dp")
    rows, width = x_h.shape
    slots = starts.shape[0]
    heads = wq_h.shape[1] // HEAD_DIM
    depth = width // STEPS
    tiles = rows // TILE
    share = width // mp
    late = slots - EARLY
    late_rows = late
    cut = rows - late * SHORTEST
    late_from = EARLY * SHORTEST

    smalls = [
        pltpu.make_async_copy(source, target, small_sem.at[i])
        for i, (source, target) in enumerate(
            [
                (gain_h, gain),
                (starts_h, starts),
                (lengths_h, lengths),
                (fine_h, fine),
                (coarse_h, coarse),
                (episode_h, episode_s),
                (flag_h, flag_s),
                (episode_h, episode_v),
                (class_h, class_v),
                (flag_h, flag_v),
            ]
        )
    ]

    bounds = [(0, depth // 2), (depth // 2, depth // 2)]
    bounds += [(depth, depth)]
    bounds += [(c * depth, 2 * depth) for c in range(2, STEPS, 2)]

    def chunk_copies(c):
        at = pl.ds(*bounds[c])
        q, k = heads * HEAD_DIM, HEAD_DIM
        return [
            pltpu.make_async_copy(
                x_h.at[:, at], x_v.at[:, at], x_sem.at[c]
            ),
            pltpu.make_async_copy(wq_h.at[at, :], w_v.at[at, pl.ds(0, q)], wq_sem.at[c]),
            pltpu.make_async_copy(wk_h.at[at, :], w_v.at[at, pl.ds(q, k)], wk_sem.at[c]),
            pltpu.make_async_copy(wv_h.at[at, :], w_v.at[at, pl.ds(q + k, k)], wv_sem.at[c]),
        ]

    smalls[0].start()
    for copy in chunk_copies(0):
        copy.start()
    for copy in smalls[1:]:
        copy.start()
    for c in range(1, AHEAD):
        for copy in chunk_copies(c):
            copy.start()
    wo_copy = pltpu.make_async_copy(wo_h, wo_v, wo_sem.at[0])

    def lane_squares(x):
        wide = x.astype(F32)
        wide = wide * wide
        total = wide[:, 0:128]
        for i in range(1, x.shape[1] // 128):
            total += wide[:, i * 128 : (i + 1) * 128]
        return total

    def project_chunk(c):
        deep = pl.ds(*bounds[c])
        for first in range(0, rows, BLOCK):
            at = pl.ds(first, BLOCK)
            x = x_v[at, deep]
            value = dot(x * gain[deep].reshape(1, bounds[c][1]), w_v[deep, :])
            if c == 0:
                squares[at, :] = lane_squares(x)
                acc[at, :] = value
            else:
                squares[at, :] += lane_squares(x)
                acc[at, :] += value

    scale = math.log2(math.e) / math.sqrt(HEAD_DIM)

    def row_scale_of(at):
        return lax.rsqrt(jnp.sum(squares[at, :], axis=1, keepdims=True) * (1.0 / width) + 1e-05)

    def slot_bounds(shape, axis):
        index = lax.broadcasted_iota(jnp.int32, shape, axis)
        first = jnp.full(shape, rows, jnp.int32)
        last = jnp.zeros(shape, jnp.int32)
        for s in range(slots):
            first = jnp.where(index == s, starts[s], first)
            last = jnp.where(index == s, starts[s] + lengths[s], last)
        return first, last

    def prepare(i):
        first, last = slot_bounds((1, 128), 1)
        fine_cos, fine_sin = fine[0], fine[1]
        at = pl.ds(i * TILE, TILE)
        row_scale = row_scale_of(at)
        cosines, sines = [], []
        for b in range(i * TILE // 64, (i + 1) * TILE // 64):
            cos_a, sin_a = coarse[0, b : b + 1, :], coarse[1, b : b + 1, :]
            cos_s, sin_s = coarse[2, b : b + 1, :], coarse[3, b : b + 1, :]
            cosines.append(cos_a * fine_cos - sin_a * fine_sin)
            sines.append(sin_s * fine_cos + cos_s * fine_sin)
        cosine = jnp.concatenate(cosines, axis=0) * row_scale
        sine = jnp.concatenate(sines, axis=0) * row_scale
        for n in range(heads):
            v = acc[at, n * 128 : (n + 1) * 128]
            v = v * cosine + pltpu.roll(v, 64, 1) * sine
            qt[i % HELD, 0:128, n * TILE : (n + 1) * TILE] = v.T.astype(BF16)
            qt[i % HELD, 128 : 128 + ONES, n * TILE : (n + 1) * TILE] = member[:, at]
        v = acc[at, heads * 128 : (heads + 1) * 128] * scale
        v = v * cosine + pltpu.roll(v, 64, 1) * sine
        ks[at, 0:128] = v.astype(BF16)
        token = i * TILE + lax.broadcasted_iota(jnp.int32, (TILE, 128), 0)
        inside = (token >= first) & (token < last)
        ks[at, 128:256] = jnp.where(inside, 0.0, FAR).astype(BF16)
        v = acc[at, (heads + 1) * 128 : (heads + 2) * 128] * row_scale
        vt[0:128, at] = v.T.astype(BF16)
        vt[128 : 128 + ONES, at] = jnp.ones((ONES, TILE), BF16)

    def score(i):
        begin = max(0, i * TILE - LONGEST)
        return dot(ks[begin : (i + 1) * TILE, :], qt[i % HELD])

    def mix(i, s):
        key = lax.broadcasted_iota(jnp.int32, (TILE, heads * TILE), 0)
        query = lax.broadcasted_iota(jnp.int32, (TILE, heads * TILE), 1) % TILE
        begin = max(0, i * TILE - LONGEST)
        before = i * TILE - begin
        own = jnp.where(key <= query, s[before:], FAR)
        peak = jnp.max(own, axis=0, keepdims=True)
        if before:
            peak = jnp.maximum(peak, jnp.max(s[:before], axis=0, keepdims=True))
        e = jnp.exp2(own - peak).astype(BF16)
        if before:
            e = jnp.concatenate([jnp.exp2(s[:before] - peak).astype(BF16), e], axis=0)
        o = dot(vt[:, begin : (i + 1) * TILE], e)
        o = (o[0:128] / o[128:129]).astype(BF16)
        for n in range(heads):
            ot[n * 128 : (n + 1) * 128, i * TILE : (i + 1) * TILE] = o[:, n * TILE : (n + 1) * TILE]

    def attend(first, last):
        prepare(first)
        ready = score(first)
        for i in range(first, last):
            now = ready
            if i + 1 < last:
                prepare(i + 1)
                ready = score(i + 1)
            mix(i, now)

    def head_part(span, pick, target):
        high, low = split(dot_nt(member[:, span], ot[:, span])[pick])
        stacked = jnp.concatenate([high, low], axis=0)
        for r in range(mp):
            both = dot(stacked, wo_v[:, r * share : (r + 1) * share])
            n = both.shape[0] // 2
            target[r] = fold(both[:n] + both[n:])

    def divided(value, first, size):
        row = lax.broadcasted_iota(jnp.int32, (value.shape[0], 1), 0)
        count = jnp.ones(row.shape, jnp.int32)
        for s in range(value.shape[0]):
            count = jnp.where(row == s, lengths[first + s % size], count)
        return value / count.astype(F32)

    order = sorted(range(1, mp), key=lambda d: -min(d, mp - d))

    def to_ranks(source, target, send, recv):
        return {
            d: pltpu.make_async_remote_copy(
                src_ref=source(d),
                dst_ref=target.at[d - 1],
                send_sem=send.at[d - 1],
                recv_sem=recv.at[d - 1],
                device_id={"mp": (me + d) % mp},
            )
            for d in order
        }

    side = int(math.isqrt(dp // 2))
    x, y, core = mine // (2 * side), (mine // 2) % side, mine % 2
    partner = mine + 1 - 2 * core

    def at_offset(dx, dy):
        return (((x + dx + side) % side) * side + (y + dy + side) % side) * 2 + core

    reach = lambda o: min(o[0], side - o[0]) + min(o[1], side - o[1])
    offsets = [(dx, dy) for dx in range(side) for dy in range(side) if dx or dy]
    offsets = sorted(offsets, key=lambda o: -reach(o))

    gathered = (everyone, late_everyone)

    def gather_copy(group, i):
        return pltpu.make_async_remote_copy(
            src_ref=gathered[group].at[mine],
            dst_ref=gathered[group].at[mine],
            send_sem=ag_send.at[group, i],
            recv_sem=ag_recv.at[group, i],
            device_id={"dp": at_offset(*offsets[i])},
        )

    def relay_copy(group, i):
        source = mine if i == len(offsets) else at_offset(-offsets[i][0], -offsets[i][1])
        return pltpu.make_async_remote_copy(
            src_ref=gathered[group].at[source],
            dst_ref=gathered[group].at[source],
            send_sem=relay_send.at[group, i],
            recv_sem=relay_recv.at[group, i],
            device_id={"dp": partner},
        )

    def gather(group):
        for i in range(len(offsets)):
            gather_copy(group, i).start()
        relay_copy(group, len(offsets)).start()

    def relay(group):
        for i in reversed(range(len(offsets))):
            gather_copy(group, i).wait_recv()
            relay_copy(group, i).start()

    barrier = pltpu.get_barrier_semaphore()
    for d in range(1, mp):
        pl.semaphore_signal(barrier, inc=1, device_id={"mp": (me + d) % mp})
    for offset in offsets:
        pl.semaphore_signal(barrier, inc=1, device_id={"dp": at_offset(*offset)})
    pl.semaphore_signal(barrier, inc=1, device_id={"dp": partner})
    smalls[0].wait()
    for c in range(len(bounds)):
        for copy in chunk_copies(c):
            copy.wait()
        if c + AHEAD < len(bounds):
            for copy in chunk_copies(c + AHEAD):
                copy.start()
        elif c + AHEAD == len(bounds):
            wo_copy.start()
        project_chunk(c)
    for copy in smalls[1:]:
        copy.wait()
    token = lax.broadcasted_iota(jnp.int32, (ONES, rows), 1)
    first, last = slot_bounds((ONES, rows), 0)
    member[...] = jnp.where((token >= first) & (token < last), 1.0, 0.0).astype(BF16)
    qt[:, 128 + ONES :, :] = jnp.zeros((HELD, 128 - ONES, heads * TILE), BF16)
    attend(0, cut // TILE)
    wo_copy.wait()
    head_part(slice(0, cut), slice(0, EARLY), part)
    pl.semaphore_wait(barrier, mp - 1 + len(offsets) + 1)
    reduce_early = to_ranks(lambda d: part.at[(me + d) % mp], landed, rs_send, rs_recv)
    for d in order:
        reduce_early[d].start()

    own_features = pl.ds(pl.multiple_of(me * share, share), share)
    pooled = fold(dot(member[:, :cut], x_v[:cut, own_features])[:EARLY])
    attend(cut // TILE, tiles)
    head_part(slice(late_from, rows), slice(EARLY, slots), late_part)
    reduce_late = to_ranks(lambda d: late_part, late_landed, ar_send, ar_recv)
    for d in order:
        reduce_late[d].start()

    pooled += part[me]
    for d in reversed(order):
        reduce_early[d].wait_recv()
        pooled += landed[d - 1]
    pooled = divided(pooled, 0, EARLY)
    everyone[mine] = pooled
    gather(0)
    late_tokens = dot(member[:, late_from:], x_v[late_from:, :])[EARLY:slots]
    for r in range(mp):
        late_total[r] = fold(late_tokens[:, r * share : (r + 1) * share]) + late_part[r]
    total = dp * slots
    classes = sums_ref.shape[0]
    named = episode_v[...] * WAYS + class_v[...]
    named = jnp.where(flag_v[...] == 0, named, -1).reshape(1, total)
    kind = lax.broadcasted_iota(jnp.int32, (classes, total), 0)
    select = jnp.where(kind == named, 1.0, 0.0).astype(BF16)
    for d in reversed(order):
        reduce_late[d].wait_recv()
    late_square = jnp.zeros((late_rows * PIECES, 1), F32)
    for r in range(mp):
        value = late_total[r]
        for d in order:
            value += late_landed[d - 1, r]
        value = divided(value, EARLY, late_rows)
        late_total[r] = value
        late_square += jnp.sum(value * value, axis=1, keepdims=True)
    lane = lax.broadcasted_iota(jnp.int32, (slots, 128), 1)
    slot = lax.broadcasted_iota(jnp.int32, (slots, 128), 0)
    late_square = jnp.sum(
        jnp.where(lane % late_rows == slot % late_rows, late_square, 0.0), axis=0, keepdims=True
    )
    late_mean = jnp.sum(
        jnp.where(lane == slot % late_rows, late_square, 0.0), axis=1, keepdims=True
    ) * (1.0 / width)
    late_own = late_total[me] * lax.rsqrt(late_mean + 1e-06)
    late_everyone[mine] = late_own
    gather(1)

    relay(0)
    for i in range(len(offsets) + 1):
        relay_copy(0, i).wait_recv()
    early = unfold(everyone[...], 0, late_rows)
    square = jnp.sum(early * early, axis=2, keepdims=True)
    wide_lane = lax.broadcasted_iota(jnp.int32, (dp, slots, 128), 2)
    wide_slot = lax.broadcasted_iota(jnp.int32, (dp, slots, 128), 1)
    square = jnp.sum(jnp.where(wide_lane == wide_slot, square, 0.0), axis=1)
    square_part[...] = square
    copies_sq = to_ranks(lambda d: square_part, square_landed, sq_send, sq_recv)
    for d in order:
        copies_sq[d].start()
    relay(1)
    for d in reversed(order):
        copies_sq[d].wait_recv()
        square += square_landed[d - 1]
    square_part_total = square.reshape(dp, 1, 128)
    mean = jnp.sum(
        jnp.where(wide_lane == wide_slot, square_part_total, 0.0), axis=2, keepdims=True
    ) * (1.0 / width)
    high, low = split((early * lax.rsqrt(mean + 1e-06)).reshape(total, share))
    sums = dot(select, high) + dot(select, low)
    own_row = lax.broadcasted_iota(jnp.int32, (dp, 128), 0) == mine
    own_square = jnp.sum(jnp.where(own_row, square, 0.0), axis=0, keepdims=True)
    own_square = jnp.where(slot >= EARLY, late_square, own_square)
    own_mean = jnp.sum(jnp.where(lane == slot, own_square, 0.0), axis=1, keepdims=True) * (
        1.0 / width
    )
    own_weight = lax.rsqrt(own_mean + 1e-06)
    own = unfold(pooled, 0, late_rows) * own_weight + unfold(late_own, EARLY, 0)
    own_high, own_low = split(own)
    own = jnp.concatenate([own_high, own_low], axis=0)
    for i in range(len(offsets) + 1):
        relay_copy(1, i).wait_recv()
    high, low = split(unfold(late_everyone[...], EARLY, 0).reshape(total, share))
    sums += dot(select, high) + dot(select, low)
    sums_high, sums_low = split(sums)
    diagonal = lax.broadcasted_iota(jnp.int32, (classes, classes), 0) == lax.broadcasted_iota(
        jnp.int32, (classes, classes), 1
    )
    norms = jnp.sum(sums * sums, axis=1, keepdims=True)
    norms = jnp.sum(jnp.where(diagonal, norms, 0.0), axis=0, keepdims=True)
    cross = dot_nt(own, sums_high)
    cross = cross[:slots] + cross[slots:] + dot_nt(own, sums_low)[:slots]
    mixed = jnp.concatenate([cross, jnp.broadcast_to(norms, (slots, classes))], axis=0)
    final_part[...] = mixed
    copies_fin = to_ranks(lambda d: final_part, final_landed, fin_send, fin_recv)
    for d in order:
        copies_fin[d].start()
    sums_ref[...] = sums
    row = lax.broadcasted_iota(jnp.int32, (slots, 1), 0)
    episode = jnp.zeros((slots, 1), jnp.int32)
    asked = jnp.zeros((slots, 1), jnp.int32)
    for s in range(slots):
        episode = jnp.where(row == s, episode_s[mine * slots + s], episode)
        asked = jnp.where(row == s, flag_s[mine * slots + s], asked)
    for copies in (reduce_early, reduce_late, copies_sq):
        for d in order:
            copies[d].wait_send()
    for group in range(2):
        for i in range(len(offsets)):
            gather_copy(group, i).wait_send()
        for i in range(len(offsets) + 1):
            relay_copy(group, i).wait_send()
    for d in reversed(order):
        copies_fin[d].wait_recv()
        mixed += final_landed[d - 1]
    class_mean = mixed[slots : slots + 1] * (1.0 / width)
    class_scale = lax.rsqrt(class_mean + 1e-06)
    column = jnp.sum(jnp.where(diagonal, class_scale, 0.0), axis=1, keepdims=True)
    column_ref[...] = jnp.broadcast_to(column, column_ref.shape)
    distance = (
        own_mean * own_weight * own_weight + class_mean * class_scale * class_scale
    ) * width - 2.0 * (mixed[:slots] * class_scale)
    picked = jnp.zeros((slots, WAYS), F32)
    for e in range(classes // WAYS):
        picked = jnp.where(episode == e, distance[:, e * WAYS : (e + 1) * WAYS], picked)
    logits = picked * (-1.0 / math.sqrt(width))
    shifted = logits - jnp.max(logits, axis=1, keepdims=True)
    result = shifted - jnp.log(jnp.sum(jnp.exp(shifted), axis=1, keepdims=True))
    log_ref[...] = jnp.where(asked == 1, result, 0.0)

    for d in order:
        copies_fin[d].wait_send()


def deliver_kernel(log_in, sums, column, log_ref, proto_ref):
    log_ref[...] = log_in[...]
    scale = column[...]
    for c in range(0, sums.shape[1], scale.shape[1]):
        at = pl.ds(c, scale.shape[1])
        proto_ref[:, at] = sums[:, at] * scale


def per_device(
    tokens,
    norm_gain,
    w_query,
    w_key,
    w_value,
    w_out,
    seq_starts,
    seq_lengths,
    episode_ids,
    class_ids,
    query_flags,
):
    rows, width = tokens.shape
    slots = seq_starts.shape[0]
    inner = w_query.shape[1]
    heads = inner // HEAD_DIM
    columns = inner + w_key.shape[1] + w_value.shape[1]
    mp, dp = lax.axis_size("mp"), lax.axis_size("dp")
    share = width // mp
    tiles = rows // TILE
    total = episode_ids.shape[0]
    classes = max(1, total // (2 * WAYS)) * WAYS
    chips = dp // 2
    late = (slots - EARLY) * PIECES
    fine, coarse = rope_tables(rows, 64)
    hbm = pl.BlockSpec(memory_space=pltpu.HBM)
    vmem = pl.BlockSpec(memory_space=pltpu.VMEM)
    dma = lambda *n: pltpu.SemaphoreType.DMA(n)
    ints = lambda n: pltpu.SMEM((n,), jnp.int32)
    log_probs, sums, column = pl.pallas_call(
        whole_kernel,
        out_shape=(
            jax.ShapeDtypeStruct((slots, WAYS), F32),
            jax.ShapeDtypeStruct((classes, share), F32),
            jax.ShapeDtypeStruct((classes, 128), F32),
        ),
        in_specs=[hbm] * 13,
        out_specs=(vmem, vmem, vmem),
        scratch_shapes=[
            ints(slots),
            ints(slots),
            ints(total),
            ints(total),
            pltpu.VMEM((total,), jnp.int32),
            pltpu.VMEM((total,), jnp.int32),
            pltpu.VMEM((total,), jnp.int32),
            pltpu.VMEM((width,), BF16),
            pltpu.VMEM(fine.shape, F32),
            pltpu.VMEM(coarse.shape, F32),
            pltpu.VMEM((rows, width), BF16),
            pltpu.VMEM((width, columns), BF16),
            pltpu.VMEM((inner, width), BF16),
            pltpu.VMEM((rows, columns), F32),
            pltpu.VMEM((rows, 128), F32),
            pltpu.VMEM((ONES, rows), BF16),
            pltpu.VMEM((HELD, 256, heads * TILE), BF16),
            pltpu.VMEM((rows, 256), BF16),
            pltpu.VMEM((128 + ONES, rows), BF16),
            pltpu.VMEM((inner, rows), BF16),
            pltpu.VMEM((mp, EARLY * PIECES, share // PIECES), F32),
            pltpu.VMEM((mp - 1, EARLY * PIECES, share // PIECES), F32),
            pltpu.VMEM((dp, EARLY * PIECES, share // PIECES), F32),
            pltpu.VMEM((mp, late, share // PIECES), F32),
            pltpu.VMEM((mp - 1, mp, late, share // PIECES), F32),
            pltpu.VMEM((mp, late, share // PIECES), F32),
            pltpu.VMEM((dp, late, share // PIECES), F32),
            pltpu.VMEM((dp, 128), F32),
            pltpu.VMEM((mp - 1, dp, 128), F32),
            pltpu.VMEM((2 * slots, 128), F32),
            pltpu.VMEM((mp - 1, 2 * slots, 128), F32),
            dma(10),
            dma(STEPS + 1),
            dma(STEPS + 1),
            dma(STEPS + 1),
            dma(STEPS + 1),
            dma(1),
            dma(mp - 1),
            dma(mp - 1),
            dma(mp - 1),
            dma(mp - 1),
            dma(mp - 1),
            dma(mp - 1),
            dma(2, chips - 1),
            dma(2, chips - 1),
            dma(2, chips),
            dma(2, chips),
            dma(mp - 1),
            dma(mp - 1),
        ],
        compiler_params=pltpu.CompilerParams(
            collective_id=0, has_side_effects=True, vmem_limit_bytes=50 * 2**20
        ),
        name="whole",
    )(
        *(
            pltpu.with_memory_space_constraint(array, pltpu.HBM)
            for array in (
                seq_starts,
                seq_lengths,
                episode_ids,
                class_ids,
                query_flags,
                norm_gain,
                jnp.asarray(fine),
                jnp.asarray(coarse),
                tokens,
                w_query,
                w_key,
                w_value,
                w_out,
            )
        )
    )
    return pl.pallas_call(
        deliver_kernel,
        out_shape=(
            jax.ShapeDtypeStruct((slots, WAYS), F32),
            jax.ShapeDtypeStruct((classes, share), F32),
        ),
        in_specs=[vmem] * 3,
        out_specs=(vmem, vmem),
        compiler_params=pltpu.CompilerParams(vmem_limit_bytes=8 * 2**20),
        name="deliver",
    )(log_probs, sums, column)


def solution(mesh):
    placed = (
        P("dp", None),
        P(),
        P(None, "mp"),
        P(None, "mp"),
        P(None, "mp"),
        P("mp", None),
        P("dp"),
        P("dp"),
        P(),
        P(),
        P(),
    )
    return jax.shard_map(
        per_device,
        mesh=mesh,
        in_specs=placed,
        out_specs=(P("dp", None), P(None, "mp")),
        check_vma=False,
    )
```

```python
import functools
import math

import jax
import jax.numpy as jnp
import numpy as np
from jax import lax
from jax.experimental import pallas as pl
from jax.experimental.pallas import tpu as pltpu
from jax.sharding import PartitionSpec as P

HEAD_DIM = 128
WAYS = 32
ROPE_BASE = 500000.0
LONGEST = 640
STEPS = 8
AHEAD = 3
HELD = 12
TILE = 128
ONES = 16
EARLY = 4
PIECES = 2
BLOCK = 512
SHORTEST = 128
FAR = -(2.0**100)
F32 = jnp.float32
BF16 = jnp.bfloat16


def rope_tables(rows, block):
    half = HEAD_DIM // 2
    frequency = ROPE_BASE ** (-(np.arange(half, dtype=np.float64) * 2.0 / HEAD_DIM))
    frequency = np.concatenate([frequency, frequency])[None, :]
    sign = np.where(np.arange(HEAD_DIM) < half, -1.0, 1.0)[None, :]
    fine = np.arange(block, dtype=np.float64)[:, None] * frequency
    coarse = np.arange(0, rows, block, dtype=np.float64)[:, None] * frequency
    fine_table = np.stack([np.cos(fine), np.sin(fine)])
    coarse_table = np.stack(
        [np.cos(coarse), np.sin(coarse), sign * np.cos(coarse), sign * np.sin(coarse)]
    )
    return fine_table.astype(np.float32), coarse_table.astype(np.float32)


def dot(a, b):
    return jnp.dot(a, b, preferred_element_type=F32)


def dot_nt(a, b):
    return lax.dot_general(a, b, (((1,), (1,)), ((), ())), preferred_element_type=F32)


def split(a):
    high = a.astype(BF16)
    return high, (a - high.astype(F32)).astype(BF16)


def fold(a):
    span = a.shape[1] // PIECES
    return jnp.concatenate([a[:, p * span : (p + 1) * span] for p in range(PIECES)], axis=0)


def unfold(a, before, after):
    axis = a.ndim - 2
    size = a.shape[axis] // PIECES
    pad = lambda n: [jnp.zeros(a.shape[:axis] + (n, a.shape[-1]), a.dtype)] if n else []
    pieces = [
        jnp.concatenate(
            pad(before)
            + [lax.slice_in_dim(a, p * size, (p + 1) * size, axis=axis)]
            + pad(after),
            axis=axis,
        )
        for p in range(PIECES)
    ]
    return jnp.concatenate(pieces, axis=axis + 1)


def whole_kernel(
    starts_h,
    lengths_h,
    episode_h,
    class_h,
    flag_h,
    gain_h,
    fine_h,
    coarse_h,
    x_h,
    wq_h,
    wk_h,
    wv_h,
    wo_h,
    log_ref,
    sums_ref,
    column_ref,
    starts,
    lengths,
    episode_s,
    flag_s,
    episode_v,
    class_v,
    flag_v,
    gain,
    fine,
    coarse,
    x_v,
    w_v,
    wo_v,
    acc,
    squares,
    member,
    qt,
    ks,
    vt,
    ot,
    part,
    landed,
    everyone,
    late_part,
    late_landed,
    late_total,
    late_everyone,
    square_part,
    square_landed,
    final_part,
    final_landed,
    small_sem,
    x_sem,
    wq_sem,
    wk_sem,
    wv_sem,
    wo_sem,
    rs_send,
    rs_recv,
    ar_send,
    ar_recv,
    sq_send,
    sq_recv,
    ag_send,
    ag_recv,
    relay_send,
    relay_recv,
    fin_send,
    fin_recv,
):
    mp = lax.axis_size("mp")
    dp = lax.axis_size("dp")
    me = lax.axis_index("mp")
    mine = lax.axis_index("dp")
    rows, width = x_h.shape
    slots = starts.shape[0]
    heads = wq_h.shape[1] // HEAD_DIM
    depth = width // STEPS
    tiles = rows // TILE
    share = width // mp
    late = slots - EARLY
    late_rows = late
    cut = rows - late * SHORTEST
    late_from = EARLY * SHORTEST

    smalls = [
        pltpu.make_async_copy(source, target, small_sem.at[i])
        for i, (source, target) in enumerate(
            [
                (gain_h, gain),
                (starts_h, starts),
                (lengths_h, lengths),
                (fine_h, fine),
                (coarse_h, coarse),
                (episode_h, episode_s),
                (flag_h, flag_s),
                (episode_h, episode_v),
                (class_h, class_v),
                (flag_h, flag_v),
            ]
        )
    ]

    bounds = [(0, depth // 2), (depth // 2, depth // 2)]
    bounds += [(depth, depth)]
    bounds += [(c * depth, 2 * depth) for c in range(2, STEPS, 2)]

    def chunk_copies(c):
        at = pl.ds(*bounds[c])
        q, k = heads * HEAD_DIM, HEAD_DIM
        return [
            pltpu.make_async_copy(
                x_h.at[:, at], x_v.at[:, at], x_sem.at[c]
            ),
            pltpu.make_async_copy(wq_h.at[at, :], w_v.at[at, pl.ds(0, q)], wq_sem.at[c]),
            pltpu.make_async_copy(wk_h.at[at, :], w_v.at[at, pl.ds(q, k)], wk_sem.at[c]),
            pltpu.make_async_copy(wv_h.at[at, :], w_v.at[at, pl.ds(q + k, k)], wv_sem.at[c]),
        ]

    smalls[0].start()
    for copy in chunk_copies(0):
        copy.start()
    for copy in smalls[1:]:
        copy.start()
    for c in range(1, AHEAD):
        for copy in chunk_copies(c):
            copy.start()
    wo_copy = pltpu.make_async_copy(wo_h, wo_v, wo_sem.at[0])

    def lane_squares(x):
        wide = x.astype(F32)
        wide = wide * wide
        total = wide[:, 0:128]
        for i in range(1, x.shape[1] // 128):
            total += wide[:, i * 128 : (i + 1) * 128]
        return total

    def project_chunk(c):
        deep = pl.ds(*bounds[c])
        for first in range(0, rows, BLOCK):
            at = pl.ds(first, BLOCK)
            x = x_v[at, deep]
            value = dot(x * gain[deep].reshape(1, bounds[c][1]), w_v[deep, :])
            if c == 0:
                squares[at, :] = lane_squares(x)
                acc[at, :] = value
            else:
                squares[at, :] += lane_squares(x)
                acc[at, :] += value

    scale = math.log2(math.e) / math.sqrt(HEAD_DIM)

    def row_scale_of(at):
        return lax.rsqrt(jnp.sum(squares[at, :], axis=1, keepdims=True) * (1.0 / width) + 1e-05)

    def slot_bounds(shape, axis):
        index = lax.broadcasted_iota(jnp.int32, shape, axis)
        first = jnp.full(shape, rows, jnp.int32)
        last = jnp.zeros(shape, jnp.int32)
        for s in range(slots):
            first = jnp.where(index == s, starts[s], first)
            last = jnp.where(index == s, starts[s] + lengths[s], last)
        return first, last

    def prepare(i):
        first, last = slot_bounds((1, 128), 1)
        fine_cos, fine_sin = fine[0], fine[1]
        at = pl.ds(i * TILE, TILE)
        row_scale = row_scale_of(at)
        cosines, sines = [], []
        for b in range(i * TILE // 64, (i + 1) * TILE // 64):
            cos_a, sin_a = coarse[0, b : b + 1, :], coarse[1, b : b + 1, :]
            cos_s, sin_s = coarse[2, b : b + 1, :], coarse[3, b : b + 1, :]
            cosines.append(cos_a * fine_cos - sin_a * fine_sin)
            sines.append(sin_s * fine_cos + cos_s * fine_sin)
        cosine = jnp.concatenate(cosines, axis=0) * row_scale
        sine = jnp.concatenate(sines, axis=0) * row_scale
        for n in range(heads):
            v = acc[at, n * 128 : (n + 1) * 128]
            v = v * cosine + pltpu.roll(v, 64, 1) * sine
            qt[i % HELD, 0:128, n * TILE : (n + 1) * TILE] = v.T.astype(BF16)
            qt[i % HELD, 128 : 128 + ONES, n * TILE : (n + 1) * TILE] = member[:, at]
        v = acc[at, heads * 128 : (heads + 1) * 128] * scale
        v = v * cosine + pltpu.roll(v, 64, 1) * sine
        ks[at, 0:128] = v.astype(BF16)
        token = i * TILE + lax.broadcasted_iota(jnp.int32, (TILE, 128), 0)
        inside = (token >= first) & (token < last)
        ks[at, 128:256] = jnp.where(inside, 0.0, FAR).astype(BF16)
        v = acc[at, (heads + 1) * 128 : (heads + 2) * 128] * row_scale
        vt[0:128, at] = v.T.astype(BF16)
        vt[128 : 128 + ONES, at] = jnp.ones((ONES, TILE), BF16)

    def score(i):
        begin = max(0, i * TILE - LONGEST)
        return dot(ks[begin : (i + 1) * TILE, :], qt[i % HELD])

    def mix(i, s):
        key = lax.broadcasted_iota(jnp.int32, (TILE, heads * TILE), 0)
        query = lax.broadcasted_iota(jnp.int32, (TILE, heads * TILE), 1) % TILE
        begin = max(0, i * TILE - LONGEST)
        before = i * TILE - begin
        own = jnp.where(key <= query, s[before:], FAR)
        peak = jnp.max(own, axis=0, keepdims=True)
        if before:
            peak = jnp.maximum(peak, jnp.max(s[:before], axis=0, keepdims=True))
        e = jnp.exp2(own - peak).astype(BF16)
        if before:
            e = jnp.concatenate([jnp.exp2(s[:before] - peak).astype(BF16), e], axis=0)
        o = dot(vt[:, begin : (i + 1) * TILE], e)
        o = (o[0:128] / o[128:129]).astype(BF16)
        for n in range(heads):
            ot[n * 128 : (n + 1) * 128, i * TILE : (i + 1) * TILE] = o[:, n * TILE : (n + 1) * TILE]

    def attend(first, last):
        prepare(first)
        ready = score(first)
        for i in range(first, last):
            now = ready
            if i + 1 < last:
                prepare(i + 1)
                ready = score(i + 1)
            mix(i, now)

    def head_part(span, pick, target):
        high, low = split(dot_nt(member[:, span], ot[:, span])[pick])
        stacked = jnp.concatenate([high, low], axis=0)
        for r in range(mp):
            both = dot(stacked, wo_v[:, r * share : (r + 1) * share])
            n = both.shape[0] // 2
            target[r] = fold(both[:n] + both[n:])

    def divided(value, first, size):
        row = lax.broadcasted_iota(jnp.int32, (value.shape[0], 1), 0)
        count = jnp.ones(row.shape, jnp.int32)
        for s in range(value.shape[0]):
            count = jnp.where(row == s, lengths[first + s % size], count)
        return value / count.astype(F32)

    order = sorted(range(1, mp), key=lambda d: -min(d, mp - d))

    def to_ranks(source, target, send, recv):
        return {
            d: pltpu.make_async_remote_copy(
                src_ref=source(d),
                dst_ref=target.at[d - 1],
                send_sem=send.at[d - 1],
                recv_sem=recv.at[d - 1],
                device_id={"mp": (me + d) % mp},
            )
            for d in order
        }

    side = int(math.isqrt(dp // 2))
    x, y, core = mine // (2 * side), (mine // 2) % side, mine % 2
    partner = mine + 1 - 2 * core

    def at_offset(dx, dy):
        return (((x + dx + side) % side) * side + (y + dy + side) % side) * 2 + core

    reach = lambda o: min(o[0], side - o[0]) + min(o[1], side - o[1])
    offsets = [(dx, dy) for dx in range(side) for dy in range(side) if dx or dy]
    offsets = sorted(offsets, key=lambda o: -reach(o))

    gathered = (everyone, late_everyone)

    def gather_copy(group, i):
        return pltpu.make_async_remote_copy(
            src_ref=gathered[group].at[mine],
            dst_ref=gathered[group].at[mine],
            send_sem=ag_send.at[group, i],
            recv_sem=ag_recv.at[group, i],
            device_id={"dp": at_offset(*offsets[i])},
        )

    def relay_copy(group, i):
        source = mine if i == len(offsets) else at_offset(-offsets[i][0], -offsets[i][1])
        return pltpu.make_async_remote_copy(
            src_ref=gathered[group].at[source],
            dst_ref=gathered[group].at[source],
            send_sem=relay_send.at[group, i],
            recv_sem=relay_recv.at[group, i],
            device_id={"dp": partner},
        )

    def gather(group):
        for i in range(len(offsets)):
            gather_copy(group, i).start()
        relay_copy(group, len(offsets)).start()

    def relay(group):
        for i in reversed(range(len(offsets))):
            gather_copy(group, i).wait_recv()
            relay_copy(group, i).start()

    barrier = pltpu.get_barrier_semaphore()
    for d in range(1, mp):
        pl.semaphore_signal(barrier, inc=1, device_id={"mp": (me + d) % mp})
    for offset in offsets:
        pl.semaphore_signal(barrier, inc=1, device_id={"dp": at_offset(*offset)})
    pl.semaphore_signal(barrier, inc=1, device_id={"dp": partner})
    smalls[0].wait()
    for c in range(len(bounds)):
        for copy in chunk_copies(c):
            copy.wait()
        if c + AHEAD < len(bounds):
            for copy in chunk_copies(c + AHEAD):
                copy.start()
        elif c + AHEAD == len(bounds):
            wo_copy.start()
        project_chunk(c)
    for copy in smalls[1:]:
        copy.wait()
    token = lax.broadcasted_iota(jnp.int32, (ONES, rows), 1)
    first, last = slot_bounds((ONES, rows), 0)
    member[...] = jnp.where((token >= first) & (token < last), 1.0, 0.0).astype(BF16)
    qt[:, 128 + ONES :, :] = jnp.zeros((HELD, 128 - ONES, heads * TILE), BF16)
    attend(0, cut // TILE)
    wo_copy.wait()
    head_part(slice(0, cut), slice(0, EARLY), part)
    pl.semaphore_wait(barrier, mp - 1 + len(offsets) + 1)
    reduce_early = to_ranks(lambda d: part.at[(me + d) % mp], landed, rs_send, rs_recv)
    for d in order:
        reduce_early[d].start()

    attend(cut // TILE, tiles)
    head_part(slice(late_from, rows), slice(EARLY, slots), late_part)
    reduce_late = to_ranks(lambda d: late_part, late_landed, ar_send, ar_recv)
    for d in order:
        reduce_late[d].start()

    own_features = pl.ds(pl.multiple_of(me * share, share), share)
    pooled = fold(dot(member[:, :cut], x_v[:cut, own_features])[:EARLY])
    pooled += part[me]
    for d in reversed(order):
        reduce_early[d].wait_recv()
        pooled += landed[d - 1]
    pooled = divided(pooled, 0, EARLY)
    everyone[mine] = pooled
    gather(0)
    late_tokens = dot(member[:, late_from:], x_v[late_from:, :])[EARLY:slots]
    for r in range(mp):
        late_total[r] = fold(late_tokens[:, r * share : (r + 1) * share]) + late_part[r]
    total = dp * slots
    classes = sums_ref.shape[0]
    named = episode_v[...] * WAYS + class_v[...]
    named = jnp.where(flag_v[...] == 0, named, -1).reshape(1, total)
    kind = lax.broadcasted_iota(jnp.int32, (classes, total), 0)
    select = jnp.where(kind == named, 1.0, 0.0).astype(BF16)
    for d in reversed(order):
        reduce_late[d].wait_recv()
    late_square = jnp.zeros((late_rows * PIECES, 1), F32)
    for r in range(mp):
        value = late_total[r]
        for d in order:
            value += late_landed[d - 1, r]
        value = divided(value, EARLY, late_rows)
        late_total[r] = value
        late_square += jnp.sum(value * value, axis=1, keepdims=True)
    lane = lax.broadcasted_iota(jnp.int32, (slots, 128), 1)
    slot = lax.broadcasted_iota(jnp.int32, (slots, 128), 0)
    late_square = jnp.sum(
        jnp.where(lane % late_rows == slot % late_rows, late_square, 0.0), axis=0, keepdims=True
    )
    late_mean = jnp.sum(
        jnp.where(lane == slot % late_rows, late_square, 0.0), axis=1, keepdims=True
    ) * (1.0 / width)
    late_own = late_total[me] * lax.rsqrt(late_mean + 1e-06)
    late_everyone[mine] = late_own
    gather(1)

    relay(0)
    for i in range(len(offsets) + 1):
        relay_copy(0, i).wait_recv()
    early = unfold(everyone[...], 0, late_rows)
    square = jnp.sum(early * early, axis=2, keepdims=True)
    wide_lane = lax.broadcasted_iota(jnp.int32, (dp, slots, 128), 2)
    wide_slot = lax.broadcasted_iota(jnp.int32, (dp, slots, 128), 1)
    square = jnp.sum(jnp.where(wide_lane == wide_slot, square, 0.0), axis=1)
    square_part[...] = square
    copies_sq = to_ranks(lambda d: square_part, square_landed, sq_send, sq_recv)
    for d in order:
        copies_sq[d].start()
    relay(1)
    for d in reversed(order):
        copies_sq[d].wait_recv()
        square += square_landed[d - 1]
    square_part_total = square.reshape(dp, 1, 128)
    mean = jnp.sum(
        jnp.where(wide_lane == wide_slot, square_part_total, 0.0), axis=2, keepdims=True
    ) * (1.0 / width)
    high, low = split((early * lax.rsqrt(mean + 1e-06)).reshape(total, share))
    sums = dot(select, high) + dot(select, low)
    own_row = lax.broadcasted_iota(jnp.int32, (dp, 128), 0) == mine
    own_square = jnp.sum(jnp.where(own_row, square, 0.0), axis=0, keepdims=True)
    own_square = jnp.where(slot >= EARLY, late_square, own_square)
    own_mean = jnp.sum(jnp.where(lane == slot, own_square, 0.0), axis=1, keepdims=True) * (
        1.0 / width
    )
    own_weight = lax.rsqrt(own_mean + 1e-06)
    own = unfold(pooled, 0, late_rows) * own_weight + unfold(late_own, EARLY, 0)
    own_high, own_low = split(own)
    own = jnp.concatenate([own_high, own_low], axis=0)
    for i in range(len(offsets) + 1):
        relay_copy(1, i).wait_recv()
    high, low = split(unfold(late_everyone[...], EARLY, 0).reshape(total, share))
    sums += dot(select, high) + dot(select, low)
    sums_high, sums_low = split(sums)
    diagonal = lax.broadcasted_iota(jnp.int32, (classes, classes), 0) == lax.broadcasted_iota(
        jnp.int32, (classes, classes), 1
    )
    norms = jnp.sum(sums * sums, axis=1, keepdims=True)
    norms = jnp.sum(jnp.where(diagonal, norms, 0.0), axis=0, keepdims=True)
    cross = dot_nt(own, sums_high)
    cross = cross[:slots] + cross[slots:] + dot_nt(own, sums_low)[:slots]
    mixed = jnp.concatenate([cross, jnp.broadcast_to(norms, (slots, classes))], axis=0)
    final_part[...] = mixed
    copies_fin = to_ranks(lambda d: final_part, final_landed, fin_send, fin_recv)
    for d in order:
        copies_fin[d].start()
    sums_ref[...] = sums
    row = lax.broadcasted_iota(jnp.int32, (slots, 1), 0)
    episode = jnp.zeros((slots, 1), jnp.int32)
    asked = jnp.zeros((slots, 1), jnp.int32)
    for s in range(slots):
        episode = jnp.where(row == s, episode_s[mine * slots + s], episode)
        asked = jnp.where(row == s, flag_s[mine * slots + s], asked)
    for copies in (reduce_early, reduce_late, copies_sq):
        for d in order:
            copies[d].wait_send()
    for group in range(2):
        for i in range(len(offsets)):
            gather_copy(group, i).wait_send()
        for i in range(len(offsets) + 1):
            relay_copy(group, i).wait_send()
    for d in reversed(order):
        copies_fin[d].wait_recv()
        mixed += final_landed[d - 1]
    class_mean = mixed[slots : slots + 1] * (1.0 / width)
    class_scale = lax.rsqrt(class_mean + 1e-06)
    column = jnp.sum(jnp.where(diagonal, class_scale, 0.0), axis=1, keepdims=True)
    column_ref[...] = jnp.broadcast_to(column, column_ref.shape)
    distance = (
        own_mean * own_weight * own_weight + class_mean * class_scale * class_scale
    ) * width - 2.0 * (mixed[:slots] * class_scale)
    picked = jnp.zeros((slots, WAYS), F32)
    for e in range(classes // WAYS):
        picked = jnp.where(episode == e, distance[:, e * WAYS : (e + 1) * WAYS], picked)
    logits = picked * (-1.0 / math.sqrt(width))
    shifted = logits - jnp.max(logits, axis=1, keepdims=True)
    result = shifted - jnp.log(jnp.sum(jnp.exp(shifted), axis=1, keepdims=True))
    log_ref[...] = jnp.where(asked == 1, result, 0.0)

    for d in order:
        copies_fin[d].wait_send()


def deliver_kernel(log_in, sums, column, log_ref, proto_ref):
    log_ref[...] = log_in[...]
    scale = column[...]
    for c in range(0, sums.shape[1], scale.shape[1]):
        at = pl.ds(c, scale.shape[1])
        proto_ref[:, at] = sums[:, at] * scale


def per_device(
    tokens,
    norm_gain,
    w_query,
    w_key,
    w_value,
    w_out,
    seq_starts,
    seq_lengths,
    episode_ids,
    class_ids,
    query_flags,
):
    rows, width = tokens.shape
    slots = seq_starts.shape[0]
    inner = w_query.shape[1]
    heads = inner // HEAD_DIM
    columns = inner + w_key.shape[1] + w_value.shape[1]
    mp, dp = lax.axis_size("mp"), lax.axis_size("dp")
    share = width // mp
    tiles = rows // TILE
    total = episode_ids.shape[0]
    classes = max(1, total // (2 * WAYS)) * WAYS
    chips = dp // 2
    late = (slots - EARLY) * PIECES
    fine, coarse = rope_tables(rows, 64)
    hbm = pl.BlockSpec(memory_space=pltpu.HBM)
    vmem = pl.BlockSpec(memory_space=pltpu.VMEM)
    dma = lambda *n: pltpu.SemaphoreType.DMA(n)
    ints = lambda n: pltpu.SMEM((n,), jnp.int32)
    log_probs, sums, column = pl.pallas_call(
        whole_kernel,
        out_shape=(
            jax.ShapeDtypeStruct((slots, WAYS), F32),
            jax.ShapeDtypeStruct((classes, share), F32),
            jax.ShapeDtypeStruct((classes, 128), F32),
        ),
        in_specs=[hbm] * 13,
        out_specs=(vmem, vmem, vmem),
        scratch_shapes=[
            ints(slots),
            ints(slots),
            ints(total),
            ints(total),
            pltpu.VMEM((total,), jnp.int32),
            pltpu.VMEM((total,), jnp.int32),
            pltpu.VMEM((total,), jnp.int32),
            pltpu.VMEM((width,), BF16),
            pltpu.VMEM(fine.shape, F32),
            pltpu.VMEM(coarse.shape, F32),
            pltpu.VMEM((rows, width), BF16),
            pltpu.VMEM((width, columns), BF16),
            pltpu.VMEM((inner, width), BF16),
            pltpu.VMEM((rows, columns), F32),
            pltpu.VMEM((rows, 128), F32),
            pltpu.VMEM((ONES, rows), BF16),
            pltpu.VMEM((HELD, 256, heads * TILE), BF16),
            pltpu.VMEM((rows, 256), BF16),
            pltpu.VMEM((128 + ONES, rows), BF16),
            pltpu.VMEM((inner, rows), BF16),
            pltpu.VMEM((mp, EARLY * PIECES, share // PIECES), F32),
            pltpu.VMEM((mp - 1, EARLY * PIECES, share // PIECES), F32),
            pltpu.VMEM((dp, EARLY * PIECES, share // PIECES), F32),
            pltpu.VMEM((mp, late, share // PIECES), F32),
            pltpu.VMEM((mp - 1, mp, late, share // PIECES), F32),
            pltpu.VMEM((mp, late, share // PIECES), F32),
            pltpu.VMEM((dp, late, share // PIECES), F32),
            pltpu.VMEM((dp, 128), F32),
            pltpu.VMEM((mp - 1, dp, 128), F32),
            pltpu.VMEM((2 * slots, 128), F32),
            pltpu.VMEM((mp - 1, 2 * slots, 128), F32),
            dma(10),
            dma(STEPS + 1),
            dma(STEPS + 1),
            dma(STEPS + 1),
            dma(STEPS + 1),
            dma(1),
            dma(mp - 1),
            dma(mp - 1),
            dma(mp - 1),
            dma(mp - 1),
            dma(mp - 1),
            dma(mp - 1),
            dma(2, chips - 1),
            dma(2, chips - 1),
            dma(2, chips),
            dma(2, chips),
            dma(mp - 1),
            dma(mp - 1),
        ],
        compiler_params=pltpu.CompilerParams(
            collective_id=0, has_side_effects=True, vmem_limit_bytes=50 * 2**20
        ),
        name="whole",
    )(
        *(
            pltpu.with_memory_space_constraint(array, pltpu.HBM)
            for array in (
                seq_starts,
                seq_lengths,
                episode_ids,
                class_ids,
                query_flags,
                norm_gain,
                jnp.asarray(fine),
                jnp.asarray(coarse),
                tokens,
                w_query,
                w_key,
                w_value,
                w_out,
            )
        )
    )
    return pl.pallas_call(
        deliver_kernel,
        out_shape=(
            jax.ShapeDtypeStruct((slots, WAYS), F32),
            jax.ShapeDtypeStruct((classes, share), F32),
        ),
        in_specs=[vmem] * 3,
        out_specs=(vmem, vmem),
        compiler_params=pltpu.CompilerParams(vmem_limit_bytes=8 * 2**20),
        name="deliver",
    )(log_probs, sums, column)


def solution(mesh):
    placed = (
        P("dp", None),
        P(),
        P(None, "mp"),
        P(None, "mp"),
        P(None, "mp"),
        P("mp", None),
        P("dp"),
        P("dp"),
        P(),
        P(),
        P(),
    )
    return jax.shard_map(
        per_device,
        mesh=mesh,
        in_specs=placed,
        out_specs=(P("dp", None), P(None, "mp")),
        check_vma=False,
    )
```
